8 devices in a mesh: rep: 4 (over z, y, x), fsdp: 2 (over core).
Axes of the slice: x: 2, y: 2, z: 1, core: 2. Of those that a mesh axis runs over, the one named last changes fastest.
Arguments:
- tok_ids: int32 [8, 512], P(('rep', 'fsdp'))
- tok_labels: int32 [8, 512], P(('rep', 'fsdp'))
- tok_pos: int32 [8, 512], P(('rep', 'fsdp'))
- expert_idx: int32 [2, 8, 512, 2], P(None, ('rep', 'fsdp'))
- learn_rate: float32 [], replicated
- embedding: float32 [32064, 512], P('fsdp')
- w_query: float32 [2, 512, 512], P(None, 'fsdp')
- w_key: float32 [2, 512, 128], P(None, 'fsdp')
- w_value: float32 [2, 512, 128], P(None, 'fsdp')
- w_attn_out: float32 [2, 512, 512], P(None, 'fsdp')
- g_attn: float32 [2, 512], P(None, 'fsdp')
- g_mlp: float32 [2, 512], P(None, 'fsdp')
- w_router: float32 [2, 512, 16], P(None, 'fsdp')
- w_gate: float32 [2, 16, 512, 800], P(None, None, 'fsdp')
- w_up: float32 [2, 16, 512, 800], P(None, None, 'fsdp')
- w_down: float32 [2, 16, 800, 512], P(None, None, 'fsdp')
- g_final: float32 [512], P('fsdp')
- w_head: float32 [512, 32064], P('fsdp')
Outputs:
- output 1: float32 [32064, 512], P('fsdp')
- output 2: float32 [2, 512, 512], P(None, 'fsdp')
- output 3: float32 [2, 512, 128], P(None, 'fsdp')
- output 4: float32 [2, 512, 128], P(None, 'fsdp')
- output 5: float32 [2, 512, 512], P(None, 'fsdp')
- output 6: float32 [2, 512], P(None, 'fsdp')
- output 7: float32 [2, 512], P(None, 'fsdp')
- output 8: float32 [2, 512, 16], P(None, 'fsdp')
- output 9: float32 [2, 16, 512, 800], P(None, None, 'fsdp')
- output 10: float32 [2, 16, 512, 800], P(None, None, 'fsdp')
- output 11: float32 [2, 16, 800, 512], P(None, None, 'fsdp')
- output 12: float32 [512], P('fsdp')
- output 13: float32 [512, 32064], P('fsdp')
- output 14: float32 [], replicated
All inputs are finite; a program needn't handle non-finite values.
Results may differ from the reference program's by a relative error of at most 0.00502737.
Values are sent between devices in bfloat16 or wider.
A program may use at most 1.25 GiB of HBM per device.

```python
import functools
import jax
import jax.numpy as jnp
from jax import lax

DIM_MODEL = 512
DIM_FF = 800
Q_HEADS = 4
KV_HEADS = 1
HEAD_DIM = 128
EXPERTS = 16
VOCAB_SIZE = 32064
BATCH_DEV = 1
SEQ_LEN = 512
BATCH_ALL = 8
LAYERS = 2
ROPE_THETA = 1000000.0
NORM_EPS = 1e-5
TOKEN_TOTAL = BATCH_ALL * SEQ_LEN
GROUP_COUNT = BATCH_ALL // BATCH_DEV


def setup_inputs(seed: int = 0) -> dict:
    keys = jax.random.split(jax.random.key(seed), 20)
    tok_shape = (BATCH_ALL, SEQ_LEN)
    route_shape = (LAYERS, BATCH_ALL, SEQ_LEN)
    q_width = Q_HEADS * HEAD_DIM
    kv_width = KV_HEADS * HEAD_DIM

    def normal(key, shape, scale):
        return jax.random.normal(key, shape, jnp.float32) * scale

    tok_ids = jax.random.randint(keys[0], tok_shape, 0, VOCAB_SIZE, dtype=jnp.int32)
    tok_labels = jax.random.randint(keys[1], tok_shape, 0, VOCAB_SIZE, dtype=jnp.int32)
    gaps = jax.random.randint(keys[2], tok_shape, 1, 4, dtype=jnp.int32)
    tok_pos = jnp.cumsum(gaps, axis=1) - gaps[:, :1]
    pick_a = jax.random.randint(keys[3], route_shape, 0, EXPERTS, dtype=jnp.int32)
    pick_b = jax.random.randint(keys[4], route_shape, 0, EXPERTS, dtype=jnp.int32)
    layer_odd = (jnp.arange(LAYERS, dtype=jnp.int32) % 2)[:, None, None]
    first = jnp.where(layer_odd == 0, jnp.minimum(pick_a, pick_b), jnp.maximum(pick_a, pick_b))
    shift = jax.random.randint(keys[5], route_shape, 1, EXPERTS, dtype=jnp.int32)
    second = (first + shift) % EXPERTS
    expert_idx = jnp.stack([first, second], axis=-1)
    learn_rate = (0.15 * TOKEN_TOTAL ** 0.5) * 2.0 ** jax.random.uniform(keys[6], (), jnp.float32, -1.0, 1.0)
    return {
        'tok_ids': tok_ids,
        'tok_labels': tok_labels,
        'tok_pos': tok_pos,
        'expert_idx': expert_idx,
        'learn_rate': learn_rate,
        'embedding': normal(keys[7], (VOCAB_SIZE, DIM_MODEL), 1.0),
        'w_query': normal(keys[8], (LAYERS, DIM_MODEL, q_width), DIM_MODEL ** -0.5),
        'w_key': normal(keys[9], (LAYERS, DIM_MODEL, kv_width), DIM_MODEL ** -0.5),
        'w_value': normal(keys[10], (LAYERS, DIM_MODEL, kv_width), DIM_MODEL ** -0.5),
        'w_attn_out': normal(keys[11], (LAYERS, q_width, DIM_MODEL), q_width ** -0.5),
        'g_attn': 1.0 + normal(keys[12], (LAYERS, DIM_MODEL), 0.3),
        'g_mlp': 1.0 + normal(keys[13], (LAYERS, DIM_MODEL), 0.3),
        'w_router': normal(keys[14], (LAYERS, DIM_MODEL, EXPERTS), DIM_MODEL ** -0.5),
        'w_gate': normal(keys[15], (LAYERS, EXPERTS, DIM_MODEL, DIM_FF), DIM_MODEL ** -0.5),
        'w_up': normal(keys[16], (LAYERS, EXPERTS, DIM_MODEL, DIM_FF), DIM_MODEL ** -0.5),
        'w_down': normal(keys[17], (LAYERS, EXPERTS, DIM_FF, DIM_MODEL), DIM_FF ** -0.5),
        'g_final': 1.0 + normal(keys[18], (DIM_MODEL,), 0.3),
        'w_head': normal(keys[19], (DIM_MODEL, VOCAB_SIZE), DIM_MODEL ** -0.5),
    }


def rms_norm(residual, gain):
    mean_sq = jnp.mean(residual * residual, axis=-1, keepdims=True)
    return (residual * lax.rsqrt(mean_sq + NORM_EPS) * gain.astype(jnp.bfloat16)).astype(jnp.bfloat16)


def rope_tables(positions):
    inv_freq = ROPE_THETA ** (-jnp.arange(0, HEAD_DIM, 2, dtype=jnp.float32) / HEAD_DIM)
    angle = positions.astype(jnp.float32)[..., None] * inv_freq
    return jnp.cos(angle)[:, :, None, :], jnp.sin(angle)[:, :, None, :]


def apply_rope(heads, cos_tab, sin_tab):
    half_dim = heads.shape[-1] // 2
    lower = heads[..., :half_dim]
    upper = heads[..., half_dim:]
    return jnp.concatenate([lower * cos_tab - upper * sin_tab, upper * cos_tab + lower * sin_tab], axis=-1)


def attention_block(normed, w_q, w_k, w_v, w_o, cos_tab, sin_tab):
    batch = normed.shape[0]
    length = normed.shape[1]
    group = Q_HEADS // KV_HEADS
    flat = normed.reshape(batch * length, DIM_MODEL)
    query = jnp.dot(flat, w_q.astype(jnp.bfloat16), preferred_element_type=jnp.float32).reshape(batch, length, Q_HEADS, HEAD_DIM)
    keyed = jnp.dot(flat, w_k.astype(jnp.bfloat16), preferred_element_type=jnp.float32).reshape(batch, length, KV_HEADS, HEAD_DIM)
    values = jnp.dot(flat, w_v.astype(jnp.bfloat16), preferred_element_type=jnp.float32).astype(jnp.bfloat16).reshape(batch, length, KV_HEADS, HEAD_DIM)
    query = apply_rope(query, cos_tab, sin_tab).astype(jnp.bfloat16).reshape(batch, length, KV_HEADS, group, HEAD_DIM)
    keyed = apply_rope(keyed, cos_tab, sin_tab).astype(jnp.bfloat16)
    scores = jnp.einsum('bqkgd,bskd->bkgqs', query.astype(jnp.float32), keyed.astype(jnp.float32)) * HEAD_DIM ** -0.5
    causal = jnp.arange(length)[:, None] >= jnp.arange(length)[None, :]
    scores = jnp.where(causal, scores, -1e30)
    attn_probs = jax.nn.softmax(scores, axis=-1).astype(jnp.bfloat16)
    mixed = jnp.einsum('bkgqs,bskd->bqkgd', attn_probs.astype(jnp.float32), values.astype(jnp.float32)).astype(jnp.bfloat16)
    mixed = mixed.reshape(batch * length, Q_HEADS * HEAD_DIM)
    projected = jnp.dot(mixed, w_o.astype(jnp.bfloat16), preferred_element_type=jnp.float32)
    return projected.reshape(batch, length, DIM_MODEL)


def moe_block(normed, w_r, w_gate, w_up, w_down, chosen):
    batch = normed.shape[0]
    length = normed.shape[1]
    flat = normed.reshape(batch * length, DIM_MODEL)
    chosen_flat = chosen.reshape(batch * length, 2)
    logits = jnp.dot(flat, w_r.astype(jnp.bfloat16), preferred_element_type=jnp.float32)
    gates = jax.nn.softmax(jnp.take_along_axis(logits, chosen_flat, axis=1), axis=-1)
    onehot = (chosen_flat[:, :, None] == jnp.arange(EXPERTS)[None, None, :]).astype(jnp.float32)
    combine = jnp.sum(gates[:, :, None] * onehot, axis=1)
    flat_wide = flat.astype(jnp.float32)
    up_a = jnp.einsum('td,xdf->xtf', flat_wide, w_gate.astype(jnp.bfloat16).astype(jnp.float32))
    up_b = jnp.einsum('td,xdf->xtf', flat_wide, w_up.astype(jnp.bfloat16).astype(jnp.float32))
    hidden = (jax.nn.silu(up_a) * up_b).astype(jnp.bfloat16)
    down = jnp.einsum('xtf,xfd->xtd', hidden.astype(jnp.float32), w_down.astype(jnp.bfloat16).astype(jnp.float32))
    mixed = jnp.einsum('tx,xtd->td', combine, down)
    return mixed.reshape(batch, length, DIM_MODEL)


def group_loss(params, group_inputs):
    ids_grp, labels_grp, pos_grp, route_grp = group_inputs
    (embedding, w_query, w_key, w_value, w_attn_out, g_attn, g_mlp, w_router, w_gate, w_up, w_down, g_final, w_head) = params
    cos_tab, sin_tab = rope_tables(pos_grp)
    residual = jnp.take(embedding.astype(jnp.bfloat16), ids_grp, axis=0).astype(jnp.float32)
    for layer in range(LAYERS):
        normed = rms_norm(residual, g_attn[layer])
        residual = residual + attention_block(normed, w_query[layer], w_key[layer], w_value[layer], w_attn_out[layer], cos_tab, sin_tab)
        normed = rms_norm(residual, g_mlp[layer])
        residual = residual + moe_block(normed, w_router[layer], w_gate[layer], w_up[layer], w_down[layer], route_grp[layer])
    final = rms_norm(residual, g_final).reshape(-1, DIM_MODEL)
    logits = jnp.dot(final, w_head.astype(jnp.bfloat16), preferred_element_type=jnp.float32)
    picked = jnp.take_along_axis(logits, labels_grp.reshape(-1, 1), axis=1)[:, 0]
    return jnp.sum(jax.nn.logsumexp(logits, axis=-1) - picked)


def reference(tok_ids, tok_labels, tok_pos, expert_idx, learn_rate, embedding, w_query, w_key, w_value, w_attn_out, g_attn, g_mlp, w_router, w_gate, w_up, w_down, g_final, w_head):
    params = (embedding, w_query, w_key, w_value, w_attn_out, g_attn, g_mlp, w_router, w_gate, w_up, w_down, g_final, w_head)
    grouped = (
        tok_ids.reshape(GROUP_COUNT, BATCH_DEV, SEQ_LEN),
        tok_labels.reshape(GROUP_COUNT, BATCH_DEV, SEQ_LEN),
        tok_pos.reshape(GROUP_COUNT, BATCH_DEV, SEQ_LEN),
        jnp.moveaxis(expert_idx.reshape(LAYERS, GROUP_COUNT, BATCH_DEV, SEQ_LEN, 2), 1, 0),
    )

    def total_loss(param_tuple):
        body = jax.checkpoint(functools.partial(group_loss, param_tuple))
        return jnp.sum(lax.map(body, grouped)) / TOKEN_TOTAL

    mean_loss, grads = jax.value_and_grad(total_loss)(params)
    updated = [master - learn_rate * gradient for master, gradient in zip(params, grads)]
    return (updated[0], updated[1], updated[2], updated[3], updated[4], updated[5], updated[6], updated[7], updated[8], updated[9], updated[10], updated[11], updated[12], mean_loss)
```

```python
import functools
import jax
import jax.numpy as jnp
from jax import lax
from jax.experimental import pallas as pl
from jax.experimental.pallas import tpu as pltpu
from jax.sharding import PartitionSpec as P

HEAD_DIM = 128
ROPE_THETA = 1000000.0
NORM_EPS = 1e-5
LOG2E = 1.4426950408889634
LN2 = 0.6931471805599453
F32 = jnp.float32
BF16 = jnp.bfloat16
I32 = jnp.int32
TILE = 16
TV = 1152
DW_STEPS = 6
SUB = 384
NEG = -1e30
ROW, COL = 0, 1
LANES = 128


def contract(a, b, ca, cb):
    return lax.dot_general(a, b, (((ca,), (cb,)), ((), ())), preferred_element_type=F32)


def dot(a, b):
    return contract(a, b, COL, ROW)


def dot_nt(a, b):
    return contract(a, b, COL, COL)


def dot_tn(a, b):
    return contract(a, b, ROW, ROW)


def get(ref):
    return ref[...]


def put(ref, value):
    ref[...] = value


def fill(ref, value):
    put(ref, jnp.full(ref.shape, value, ref.dtype))


def iota(shape, axis):
    return lax.broadcasted_iota(I32, shape, axis)


def axis_sum(x, axis):
    return jnp.sum(x, axis=axis, keepdims=True)


def keep(mask, x):
    return jnp.where(mask, x, 0.0)


def hot(mask):
    return jnp.where(mask, 1.0, 0.0).astype(BF16)


def lane_groups(x):
    return jnp.split(x, x.shape[COL] // LANES, axis=COL)


def pair_of(x, axis):
    return jnp.split(x, 2, axis=axis)


def side_by_side(ref):
    return jnp.concatenate([ref[core].reshape(ref.shape[-2:]) for core in range(2)], axis=COL)


def rms_stats(x):
    return lax.rsqrt(jnp.mean(x * x, axis=-1, keepdims=True) + NORM_EPS)


def rms_norm(x, gain):
    return (x * rms_stats(x) * gain).astype(BF16)


def rms_norm_bwd(x, gain, d_normed):
    inv = rms_stats(x)
    unit = x * inv
    d_gain = axis_sum(d_normed * unit, ROW)
    d_unit = d_normed * gain
    d_x = inv * (d_unit - unit * jnp.mean(d_unit * unit, axis=-1, keepdims=True))
    return d_x, d_gain


def split3(x):
    hi = x.astype(BF16)
    rest = x - hi.astype(F32)
    mid = rest.astype(BF16)
    return hi, mid, (rest - mid.astype(F32)).astype(BF16)


def select_rows(onehot, x):
    hi, mid, lo = split3(x)
    return dot(onehot, hi) + dot(onehot, mid) + dot(onehot, lo)


def params(vmem_mib, **kw):
    return pltpu.CompilerParams(vmem_limit_bytes=vmem_mib << 20, **kw)


def whole(shape):
    zeros = (0,) * len(shape)
    return pl.BlockSpec(shape, lambda *_: zeros)


def route_masks(pos_row, rows):
    return [iota((rows, pos.shape[COL]), ROW) == pos for pos in pair_of(pos_row, ROW)]


def moe_fwd_kernel(off, x_ref, gain_ref, wr_ref, prow_ref, pcol_ref, ecol_ref, wg_ref, wu_ref, wd_ref,
                   out_ref, xs_out, y0_out, y1_out, xs_s, down_s, *, rows, blk):
    expert = pl.program_id(0)
    toks = x_ref.shape[0]

    @pl.when(expert == 0)
    def _():
        normed = rms_norm(get(x_ref), get(gain_ref))
        hit0, hit1 = route_masks(get(prow_ref), rows)
        spread = hot(hit0 | hit1)
        xs = dot(spread, normed).astype(BF16)
        put(xs_out, xs)
        xs_s[pl.ds(0, rows), :] = xs
        xs_s[pl.ds(rows, blk), :] = jnp.zeros((blk, xs.shape[1]), BF16)
        fill(down_s, 0)

    w_gate = side_by_side(wg_ref)
    w_up = side_by_side(wu_ref)
    w_down = get(wd_ref).reshape(w_gate.shape)
    start = off[expert]
    count = off[expert + 1] - start

    def body(i, carry):
        at = pl.multiple_of(start + i * blk, TILE)
        xs = xs_s[pl.ds(at, blk), :]
        gate = dot_nt(w_gate, xs)
        up = dot_nt(w_up, xs)
        hidden = (gate * jax.nn.sigmoid(gate) * up).astype(BF16)
        down_s[pl.ds(at, blk), :] = dot_tn(hidden, w_down)
        return carry

    lax.fori_loop(0, (count + blk - 1) // blk, body, 0)

    @pl.when(expert == pl.num_programs(0) - 1)
    def _():
        x = get(x_ref)
        normed = rms_norm(x, get(gain_ref))
        logits = dot_nt(normed, get(wr_ref))
        gate0, gate1 = pair_gates(logits, get(ecol_ref), COL)
        col_id = iota((toks, rows), COL)
        slot0, slot1 = pair_of(get(pcol_ref), COL)
        pick0 = hot(col_id == slot0)
        pick1 = hot(col_id == slot1)
        hi, mid, lo = split3(down_s[pl.ds(0, rows), :])
        y0 = dot(pick0, hi) + dot(pick0, mid) + dot(pick0, lo)
        y1 = dot(pick1, hi) + dot(pick1, mid) + dot(pick1, lo)
        put(y0_out, y0)
        put(y1_out, y1)
        put(out_ref, x + (y0 * gate0 + y1 * gate1))


def pair_gates(logits, experts, axis):
    ids = iota(logits.shape, axis)
    r0, r1 = [axis_sum(keep(ids == chosen, logits), axis) for chosen in pair_of(experts, axis)]
    top = jnp.maximum(r0, r1)
    e0 = jnp.exp(r0 - top)
    e1 = jnp.exp(r1 - top)
    return e0 / (e0 + e1), e1 / (e0 + e1)


def moe_bwd_kernel(off, dx_ref, x_ref, gain_ref, wr_ref, prow_ref, pcol_ref, erow_ref, ecol_ref, y0_ref, y1_ref, xs_ref, extra_ref,
                   wg_ref, wu_ref, wd_ref, dx_out, dys_out, dwr_out, dg_out, xs_s, dys_s, dxs_s, *, rows, blk):
    expert = pl.program_id(0)
    toks, width = x_ref.shape

    @pl.when(expert == 0)
    def _():
        dx = get(dx_ref)
        normed = rms_norm(get(x_ref), get(gain_ref))
        logits_t = dot_nt(get(wr_ref), normed)
        gate0, gate1 = pair_gates(logits_t, get(erow_ref), ROW)
        hit0, hit1 = route_masks(get(prow_ref), rows)
        spread = hot(hit0 | hit1)
        gate_rows = axis_sum(keep(hit0, gate0) + keep(hit1, gate1), COL)
        dys = select_rows(spread, dx) * gate_rows
        dys_out[pl.ds(0, rows), :] = dys
        dys_out[pl.ds(rows, 8), :] = get(extra_ref)
        dys_s[pl.ds(0, rows), :] = dys.astype(BF16)
        dys_s[pl.ds(rows, blk), :] = jnp.zeros((blk, width), BF16)
        xs_s[pl.ds(0, rows), :] = get(xs_ref)
        xs_s[pl.ds(rows, blk), :] = jnp.zeros((blk, width), BF16)
        fill(dxs_s, 0)

    w_gate = side_by_side(wg_ref)
    w_up = side_by_side(wu_ref)
    w_down = get(wd_ref).reshape(w_gate.shape)
    start = off[expert]
    count = off[expert + 1] - start

    def body(i, carry):
        at = pl.multiple_of(start + i * blk, TILE)
        xs = xs_s[pl.ds(at, blk), :]
        dys = dys_s[pl.ds(at, blk), :]
        gate = dot_nt(w_gate, xs)
        up = dot_nt(w_up, xs)
        d_hidden = dot_nt(w_down, dys)
        d_gate, d_up, _ = glu_bwd(gate, up, d_hidden)
        dxs_s[pl.ds(at, blk), :] = dot_tn(d_gate, w_gate) + dot_tn(d_up, w_up)
        return carry

    lax.fori_loop(0, (count + blk - 1) // blk, body, 0)

    @pl.when(expert == pl.num_programs(0) - 1)
    def _():
        x = get(x_ref)
        dx = get(dx_ref)
        gain = get(gain_ref)
        normed = rms_norm(x, gain)
        logits = dot_nt(normed, get(wr_ref))
        experts = get(ecol_ref)
        gate0, gate1 = pair_gates(logits, experts, COL)
        d_gate0 = axis_sum(dx * get(y0_ref), COL)
        d_gate1 = axis_sum(dx * get(y1_ref), COL)
        mean = gate0 * d_gate0 + gate1 * d_gate1
        first, second = pair_of(experts, COL)
        ids = iota(logits.shape, COL)
        d_logits = (keep(ids == first, gate0 * (d_gate0 - mean)) + keep(ids == second, gate1 * (d_gate1 - mean))).astype(BF16)
        put(dwr_out, dot_tn(d_logits, normed))
        col_id = iota((toks, rows), COL)
        slot0, slot1 = pair_of(get(pcol_ref), COL)
        collect = hot((col_id == slot0) | (col_id == slot1))
        d_normed = select_rows(collect, dxs_s[pl.ds(0, rows), :]) + dot(d_logits, get(wr_ref))
        d_x, d_gain = rms_norm_bwd(x, gain, d_normed.astype(BF16).astype(F32))
        put(dx_out, dx + d_x)
        put(dg_out, d_gain)


def glu_bwd(gate, up, d_hidden):
    sig = jax.nn.sigmoid(gate)
    act = gate * sig
    d_gate = (d_hidden * up * (sig + act * (1.0 - sig))).astype(BF16)
    d_up = (d_hidden * act).astype(BF16)
    return d_gate, d_up, act


def expert_specs(experts, ff, half):
    up_spec = pl.BlockSpec((2, 1, ff, half), lambda e, *_: (0, e, 0, 0))
    down_spec = pl.BlockSpec((2, 1, ff // 2, 2 * half), lambda e, *_: (0, e, 0, 0))
    return [up_spec, up_spec, down_spec]


def moe_fwd(off, x, gain, w_r, pos_row, pos_col, exp_col, w_gate, w_up, w_down, rows):
    toks, width = x.shape
    experts, ff = w_gate.shape[1], w_gate.shape[2]
    blk = 128
    tok_out = jax.ShapeDtypeStruct((toks, width), F32)
    small = [x, gain, w_r, pos_row, pos_col, exp_col]
    return pl.pallas_call(
        functools.partial(moe_fwd_kernel, rows=rows, blk=blk),
        out_shape=(tok_out, jax.ShapeDtypeStruct((rows, width), BF16), tok_out, tok_out),
        grid_spec=pltpu.PrefetchScalarGridSpec(
            num_scalar_prefetch=1,
            grid=(experts,),
            in_specs=[whole(a.shape) for a in small] + expert_specs(experts, ff, width // 2),
            out_specs=(whole((toks, width)), whole((rows, width)), whole((toks, width)), whole((toks, width))),
            scratch_shapes=[pltpu.VMEM((rows + blk, width), BF16), pltpu.VMEM((rows + blk, width), F32)],
        ),
        compiler_params=params(48),
        cost_estimate=pl.CostEstimate(flops=30_000_000_000, bytes_accessed=45_000_000, transcendentals=0),
        name="moe_fwd",
    )(off, *small, w_gate, w_up, w_down)


def moe_bwd(off, dx, x, gain, w_r, pos_row, pos_col, exp_row, exp_col, y0, y1, xs, extra, w_gate, w_up, w_down, rows):
    toks, width = x.shape
    experts, ff = w_gate.shape[1], w_gate.shape[2]
    blk = 128
    small = [dx, x, gain, w_r, pos_row, pos_col, exp_row, exp_col, y0, y1, xs, extra]
    out_shapes = (
        jax.ShapeDtypeStruct((toks, width), F32),
        jax.ShapeDtypeStruct((rows + 8, width), F32),
        jax.ShapeDtypeStruct((experts, width), F32),
        jax.ShapeDtypeStruct((1, width), F32),
    )
    return pl.pallas_call(
        functools.partial(moe_bwd_kernel, rows=rows, blk=blk),
        out_shape=out_shapes,
        grid_spec=pltpu.PrefetchScalarGridSpec(
            num_scalar_prefetch=1,
            grid=(experts,),
            in_specs=[whole(a.shape) for a in small] + expert_specs(experts, ff, width // 2),
            out_specs=tuple(whole(s.shape) for s in out_shapes),
            scratch_shapes=[
                pltpu.VMEM((rows + blk, width), BF16),
                pltpu.VMEM((rows + blk, width), BF16),
                pltpu.VMEM((rows + blk, width), F32),
            ],
        ),
        compiler_params=params(60),
        cost_estimate=pl.CostEstimate(flops=50_000_000_000, bytes_accessed=50_000_000, transcendentals=0),
        name="moe_bwd",
    )(off, *small, w_gate, w_up, w_down)


def expert_dw_kernel(off, fs, lr_ref, xs_hbm, dys_hbm, wg_ref, wu_ref, wd_ref, mg_ref, mu_ref, md_ref, *refs, blk, alias):
    refs = refs[3:] if alias else refs
    og_ref, ou_ref, od_ref, xbuf, dbuf, sems, acc_g, acc_u, acc_d = refs
    expert = pl.program_id(0)
    experts = pl.num_programs(0)
    seqs = xs_hbm.shape[0]
    ff, half = acc_g.shape
    mine = fs[0]

    def copies(e, slot, go):
        at = 0
        for s in range(seqs):
            start = pl.multiple_of(off[s, e], TILE)
            count = pl.multiple_of(off[s, e + 1] - off[s, e], TILE)
            dst = pl.multiple_of(at, TILE)

            @pl.when(count > 0)
            def _():
                for hbm, buf, k in ((xs_hbm, xbuf, 0), (dys_hbm, dbuf, 1)):
                    copy = pltpu.make_async_copy(hbm.at[s, pl.ds(start, count), :], buf.at[slot, pl.ds(dst, count), :], sems.at[slot, k])
                    if go:
                        copy.start()
                    else:
                        copy.wait()

            at = at + count
        return at

    slot = lax.rem(expert, 2)

    @pl.when(expert == 0)
    def _():
        copies(0, 0, True)

    @pl.when(expert + 1 < experts)
    def _():
        copies(expert + 1, 1 - slot, True)

    total = pl.multiple_of(copies(expert, slot, False), TILE)
    xbuf[slot, pl.ds(total, blk), :] = jnp.zeros((blk, xbuf.shape[2]), BF16)
    dbuf[slot, pl.ds(total, blk), :] = jnp.zeros((blk, dbuf.shape[2]), F32)
    fill(acc_g, 0)
    fill(acc_u, 0)
    fill(acc_d, 0)
    w_gate = side_by_side(wg_ref)
    w_up = side_by_side(wu_ref)
    w_down = get(wd_ref).reshape(w_gate.shape)

    def body(i, carry):
        at = pl.multiple_of(i * blk, blk)
        xs = xbuf[slot, pl.ds(at, blk), :]
        own = xbuf[slot, pl.ds(at, blk), pl.ds(pl.multiple_of(mine * half, half), half)]
        dys = dbuf[slot, pl.ds(at, blk), :].astype(BF16)
        gate = dot_nt(w_gate, xs)
        up = dot_nt(w_up, xs)
        d_hidden = dot_nt(w_down, dys)
        d_gate, d_up, act = glu_bwd(gate, up, d_hidden)
        hidden = (act * up).astype(BF16)
        put(acc_g, get(acc_g) + dot(d_gate, own))
        put(acc_u, get(acc_u) + dot(d_up, own))
        hidden_own = jnp.where(mine == 0, hidden[: ff // 2], hidden[ff // 2 :])
        put(acc_d, get(acc_d) + dot(hidden_own, dys))
        return carry

    lax.fori_loop(0, (total + blk - 1) // blk, body, 0)
    for out, master, acc in ((og_ref, mg_ref, acc_g), (ou_ref, mu_ref, acc_u), (od_ref, md_ref, acc_d)):
        put(out, get(master) - get(lr_ref) * get(acc).reshape(out.shape))


def expert_dw(layer, off, fs, lr, xs, dys, w_gate, w_up, w_down, m_gate, m_up, m_down, prev):
    seqs, _, width = xs.shape
    layers, experts, ff, half = m_gate.shape
    blk = 256
    most = seqs * ((width + TILE - 1) // TILE * TILE)
    any_spec = pl.BlockSpec(memory_space=pl.ANY)
    up_master = pl.BlockSpec((1, 1, ff, half), lambda e, *_: (layer, e, 0, 0))
    down_master = pl.BlockSpec((1, 1, ff // 2, width), lambda e, *_: (layer, e, 0, 0))
    masters = [up_master, up_master, down_master]
    alias = prev is not None
    in_specs = [whole(lr.shape), any_spec, any_spec] + expert_specs(experts, ff, half) + masters
    in_specs += [any_spec] * 3 if alias else []
    return pl.pallas_call(
        functools.partial(expert_dw_kernel, blk=blk, alias=alias),
        out_shape=tuple(jax.ShapeDtypeStruct(m.shape, F32) for m in (m_gate, m_up, m_down)),
        grid_spec=pltpu.PrefetchScalarGridSpec(
            num_scalar_prefetch=2,
            grid=(experts,),
            in_specs=in_specs,
            out_specs=tuple(masters),
            scratch_shapes=[
                pltpu.VMEM((2, most + blk, width), BF16),
                pltpu.VMEM((2, most + blk, width), F32),
                pltpu.SemaphoreType.DMA((2, 2)),
                pltpu.VMEM((ff, half), F32),
                pltpu.VMEM((ff, half), F32),
                pltpu.VMEM((ff // 2, width), F32),
            ],
        ),
        input_output_aliases={11: 0, 12: 1, 13: 2} if alias else {},
        compiler_params=params(62),
        cost_estimate=pl.CostEstimate(flops=90_000_000_000, bytes_accessed=150_000_000, transcendentals=0),
        name="expert_dw",
    )(off, fs, lr, xs, dys, w_gate, w_up, w_down, m_gate, m_up, m_down, *(prev or ()))


def head_kernel(x_ref, gain_ref, lab_ref, w_ref, fin_out, lse_out, dx_out, dg_out, loss_out, top_s, sum_s, pick_s, acc_s, *, vocab, tokens_all):
    sweep = pl.program_id(0)
    step = pl.program_id(1)
    last = pl.num_programs(1) - 1
    toks = x_ref.shape[0]
    tile = w_ref.shape[1]

    @pl.when((sweep == 0) & (step == 0))
    def _():
        put(fin_out, rms_norm(get(x_ref), get(gain_ref)))
        fill(top_s, NEG)
        fill(sum_s, 0)
        fill(pick_s, 0)
        fill(acc_s, 0)

    weights = side_by_side(w_ref)
    col = iota((1, tile), COL) + step * tile
    bias = jnp.where(col < vocab, 0.0, NEG)
    logits = dot_nt(get(fin_out), weights) * LOG2E + bias

    @pl.when(sweep == 0)
    def _():
        parts = lane_groups(logits)
        old = get(top_s)
        new = functools.reduce(jnp.maximum, parts, old)
        put(sum_s, functools.reduce(jnp.add, [jnp.exp2(p - new) for p in parts], get(sum_s) * jnp.exp2(old - new)))
        put(top_s, new)

    @pl.when((sweep == 0) & (step == last))
    def _():
        top = jnp.max(get(top_s), axis=COL, keepdims=True)
        total = axis_sum(get(sum_s) * jnp.exp2(get(top_s) - top), COL)
        put(lse_out, top + jnp.log2(total))

    @pl.when(sweep == 1)
    def _():
        prob = jnp.exp2(logits - (get(lse_out) + jnp.log2(jnp.float32(tokens_all))))
        hit = iota((toks, tile), COL) == get(lab_ref) - step * tile
        grad = (prob - jnp.where(hit, 1.0 / tokens_all, 0.0)).astype(BF16)
        picked = jnp.where(hit, logits, 0.0)
        put(pick_s, get(pick_s) + functools.reduce(jnp.add, lane_groups(picked)))
        put(acc_s, get(acc_s) + dot(grad, weights))

    @pl.when((sweep == 1) & (step == last))
    def _():
        per_tok = (get(lse_out) - axis_sum(get(pick_s), COL)) * (LN2 / tokens_all)
        put(loss_out, jnp.broadcast_to(axis_sum(per_tok, ROW), loss_out.shape))
        d_x, d_gain = rms_norm_bwd(get(x_ref), get(gain_ref), get(acc_s).astype(BF16).astype(F32))
        put(dx_out, d_x)
        put(dg_out, d_gain)


def head(x, gain, labels, w_head, vocab, tokens_all):
    toks, width = x.shape
    steps = w_head.shape[1] // TV
    out_shapes = (
        jax.ShapeDtypeStruct((toks, width), BF16),
        jax.ShapeDtypeStruct((toks, 1), F32),
        jax.ShapeDtypeStruct((toks, width), F32),
        jax.ShapeDtypeStruct((1, width), F32),
        jax.ShapeDtypeStruct((1, width), F32),
    )
    small = [x, gain, labels]
    return pl.pallas_call(
        functools.partial(head_kernel, vocab=vocab, tokens_all=tokens_all),
        out_shape=out_shapes,
        grid=(2, steps),
        in_specs=[whole(a.shape) for a in small] + [pl.BlockSpec((2, TV, width // 2), lambda p, i: (0, i, 0))],
        out_specs=tuple(whole(s.shape) for s in out_shapes),
        scratch_shapes=[pltpu.VMEM((toks, LANES), F32)] * 3 + [pltpu.VMEM((toks, width), F32)],
        compiler_params=params(48),
        cost_estimate=pl.CostEstimate(flops=55_000_000_000, bytes_accessed=70_000_000, transcendentals=0),
        name="head_own",
    )(*small, w_head)


def head_dw_kernel(fs, lr_ref, fin_ref, lse_ref, lab_ref, w_ref, m_ref, new_out, oth_out, acc_s, *, tokens_all):
    tile = w_ref.shape[1]
    half = m_ref.shape[1]
    mine = fs[0]
    first = (mine * pl.num_programs(0) + pl.program_id(0)) * tile
    weights = side_by_side(w_ref)
    fill(acc_s, 0)
    edges = list(range(0, tile, SUB)) + [tile]

    def body(s, carry):
        fin = fin_ref[s]
        lse = lse_ref[s] + jnp.log2(jnp.float32(tokens_all))
        lab = lab_ref[s] - first
        for lo, hi in zip(edges, edges[1:]):
            logits = dot_nt(weights[lo:hi], fin) * LOG2E
            hit = iota(logits.shape, ROW) == lab - lo
            grad = (jnp.exp2(logits - lse) - jnp.where(hit, 1.0 / tokens_all, 0.0)).astype(BF16)
            acc_s[lo:hi] += dot(grad, fin)
        return carry

    lax.fori_loop(0, fin_ref.shape[0], body, 0)
    own = acc_s[:, pl.ds(pl.multiple_of(mine * half, half), half)]
    put(new_out, get(m_ref) - get(lr_ref) * own)
    put(oth_out, acc_s[:, pl.ds(pl.multiple_of((1 - mine) * half, half), half)])


def head_dw(fs, lr, fin, lse, labels, w_head, master, tokens_all):
    seqs, toks, width = fin.shape
    vocab, half = master.shape
    steps = DW_STEPS
    tile = vocab // 2 // steps
    tile_of = lambda i, f, *_: f[0] * steps + i
    return pl.pallas_call(
        functools.partial(head_dw_kernel, tokens_all=tokens_all),
        out_shape=(jax.ShapeDtypeStruct((vocab, half), F32), jax.ShapeDtypeStruct((steps * tile, half), F32)),
        grid_spec=pltpu.PrefetchScalarGridSpec(
            num_scalar_prefetch=1,
            grid=(steps,),
            in_specs=[
                whole(lr.shape),
                whole(fin.shape),
                whole(lse.shape),
                whole(labels.shape),
                pl.BlockSpec((2, tile, half), lambda i, f: (0, tile_of(i, f), 0)),
                pl.BlockSpec((tile, half), lambda i, f: (tile_of(i, f), 0)),
            ],
            out_specs=(
                pl.BlockSpec((tile, half), lambda i, f: (tile_of(i, f), 0)),
                pl.BlockSpec((tile, half), lambda i, f: (i, 0)),
            ),
            scratch_shapes=[pltpu.VMEM((tile, width), F32)],
        ),
        compiler_params=params(56),
        cost_estimate=pl.CostEstimate(flops=140_000_000_000, bytes_accessed=70_000_000, transcendentals=0),
        name="head_dw",
    )(fs, lr, fin, lse, labels, w_head, master)


def head_upd_kernel(fs, lr_ref, grad_ref, m_ref, prev_ref, new_out):
    put(new_out, get(m_ref) - get(lr_ref) * get(grad_ref))


def head_upd(fs, lr, grad, master, prev):
    vocab, half = master.shape
    steps = DW_STEPS
    tile = grad.shape[0] // steps
    spec = pl.BlockSpec((tile, half), lambda i, f: ((1 - f[0]) * steps + i, 0))
    return pl.pallas_call(
        head_upd_kernel,
        out_shape=jax.ShapeDtypeStruct((vocab, half), F32),
        grid_spec=pltpu.PrefetchScalarGridSpec(
            num_scalar_prefetch=1,
            grid=(steps,),
            in_specs=[
                whole(lr.shape),
                pl.BlockSpec((tile, half), lambda i, f: (i, 0)),
                spec,
                pl.BlockSpec(memory_space=pl.ANY),
            ],
            out_specs=spec,
        ),
        input_output_aliases={4: 0},
        compiler_params=params(32),
        cost_estimate=pl.CostEstimate(flops=15_000_000_000, bytes_accessed=50_000_000, transcendentals=0),
        name="head_upd",
    )(fs, lr, grad, master, prev)


def embed_upd_kernel(bounds, keys, perm, lr_ref, rows_ref, m_ref, new_out, wide_s):
    step = pl.program_id(0)
    rows = m_ref.shape[0]

    @pl.when(step == 0)
    def _():
        put(wide_s, get(rows_ref).astype(F32) * get(lr_ref))

    put(new_out, get(m_ref))

    def body(j, carry):
        at = new_out.at[pl.ds(keys[j] - step * rows, 1)]
        put(at, get(at) - get(wide_s.at[pl.ds(perm[j], 1)]))
        return carry

    lax.fori_loop(bounds[step], bounds[step + 1], body, 0)


def embed_upd(bounds, keys, perm, lr, grads, master, rows):
    vocab, width = master.shape
    return pl.pallas_call(
        embed_upd_kernel,
        out_shape=jax.ShapeDtypeStruct((vocab, width), F32),
        grid_spec=pltpu.PrefetchScalarGridSpec(
            num_scalar_prefetch=3,
            grid=(vocab // rows,),
            in_specs=[
                whole(lr.shape),
                whole(grads.shape),
                pl.BlockSpec((rows, width), lambda i, *_: (i, 0)),
            ],
            out_specs=pl.BlockSpec((rows, width), lambda i, *_: (i, 0)),
            scratch_shapes=[pltpu.VMEM(grads.shape, F32)],
        ),
        compiler_params=params(48),
        cost_estimate=pl.CostEstimate(flops=25_000_000_000, bytes_accessed=66_000_000, transcendentals=0),
        name="embed_upd",
    )(bounds, keys, perm, lr, grads, master)


def rope_tables(positions):
    inv_freq = ROPE_THETA ** (-jnp.arange(0, HEAD_DIM, 2, dtype=F32) / HEAD_DIM)
    angle = positions.astype(F32)[..., None] * inv_freq
    return jnp.cos(angle)[:, None, :], jnp.sin(angle)[:, None, :]


def apply_rope(heads, cos_tab, sin_tab):
    half_dim = heads.shape[-1] // 2
    lower = heads[..., :half_dim]
    upper = heads[..., half_dim:]
    return jnp.concatenate([lower * cos_tab - upper * sin_tab, upper * cos_tab + lower * sin_tab], axis=-1)


def attention(x, gain, w_all, cos_tab, sin_tab, q_width, kv_width):
    length = x.shape[0]
    q_heads = q_width // HEAD_DIM
    w_q, w_k, w_v, w_o = jnp.split(w_all, (q_width, q_width + kv_width, q_width + 2 * kv_width), axis=1)
    normed = rms_norm(x, gain)
    query = dot(normed, w_q).reshape(length, q_heads, HEAD_DIM)
    keyed = dot(normed, w_k).reshape(length, 1, HEAD_DIM)
    values = dot(normed, w_v).astype(BF16)
    query = apply_rope(query, cos_tab, sin_tab).astype(BF16)
    keyed = apply_rope(keyed, cos_tab, sin_tab).astype(BF16)[:, 0]
    scores = jnp.einsum('qgd,sd->gqs', query, keyed, preferred_element_type=F32) * HEAD_DIM ** -0.5
    causal = iota((length, length), 0) >= iota((length, length), 1)
    scores = jnp.where(causal, scores, NEG)
    probs = jax.nn.softmax(scores, axis=-1).astype(BF16)
    mixed = jnp.einsum('gqs,sd->qgd', probs, values, preferred_element_type=F32).astype(BF16).reshape(length, q_width)
    return x + dot(mixed, w_o)


def routing(experts_of, experts):
    toks = experts_of.shape[0]
    hot = (experts_of[:, :, None] == jnp.arange(experts, dtype=I32)).astype(F32)
    both = hot[:, 0] + hot[:, 1]
    before = iota((toks, toks), 0) > iota((toks, toks), 1)
    ahead = dot(before.astype(BF16), both.astype(BF16))
    counts = jnp.sum(both, axis=0).astype(I32)
    padded = (counts + TILE - 1) // TILE * TILE
    upto = iota((experts + 1, experts), 0) > iota((experts + 1, experts), 1)
    starts = jnp.sum(jnp.where(upto, padded[None, :], 0), axis=1)
    place = starts[:experts].astype(F32) + ahead
    return jnp.sum(hot * place[:, None, :], axis=2).astype(I32), starts


def solution(mesh):
    device_count = mesh.shape['rep'] * mesh.shape['fsdp']
    both = ('rep', 'fsdp')
    batch_spec = P(both)
    layer_spec = P(None, 'fsdp')
    expert_spec = P(None, None, 'fsdp')
    param_specs = (P('fsdp'), layer_spec, layer_spec, layer_spec, layer_spec, layer_spec, layer_spec, layer_spec, expert_spec, expert_spec, expert_spec, P('fsdp'), P('fsdp'))
    in_specs = (batch_spec, batch_spec, batch_spec, P(None, both), P()) + param_specs
    out_specs = param_specs + (P(),)

    def step(tok_ids, tok_labels, tok_pos, expert_idx, learn_rate, embedding, w_query, w_key, w_value, w_attn_out, g_attn, g_mlp, w_router, w_gate, w_up, w_down, g_final, w_head):
        layers, half, q_width = w_query.shape
        kv_width = w_key.shape[2]
        width = 2 * half
        toks = tok_ids.shape[1]
        experts = w_router.shape[2]
        tokens_all = toks * device_count
        vocab_share = embedding.shape[0]
        vocab = w_head.shape[1]
        rows = 2 * toks + experts * TILE
        me = lax.axis_index('fsdp')
        pair = lax.axis_index('rep')
        fs = me.astype(I32).reshape(1)
        lr = learn_rate.reshape(1, 1)
        swap = [(0, 1), (1, 0)]

        m_gate = jnp.swapaxes(w_gate, 2, 3)
        m_up = jnp.swapaxes(w_up, 2, 3)
        m_head = w_head.T

        experts_of = expert_idx[:, 0]
        placed = [routing(experts_of[l], experts) for l in range(layers)]
        starts = jnp.stack([s for _, s in placed])
        ints = jnp.concatenate([tok_ids[0], tok_labels[0], starts.reshape(-1)]).astype(F32)
        misc = jnp.concatenate([jnp.swapaxes(w_router, 1, 2).reshape(layers * experts, half), g_attn, g_mlp, g_final[None]])
        misc = misc.astype(BF16).astype(F32).reshape(-1)
        packed = jnp.concatenate([misc, ints])
        n_misc = misc.shape[0]
        packed = jnp.pad(packed, (0, -packed.shape[0] % 1024)).reshape(-1, 128)
        known = lax.all_gather(packed, both).reshape(device_count, -1)
        two = lax.dynamic_slice_in_dim(known, pair * 2, 2, 0)[:, :n_misc].reshape(2, -1, half)
        misc_all = jnp.concatenate([two[0], two[1]], axis=1)
        w_r = [misc_all[l * experts : (l + 1) * experts].astype(BF16) for l in range(layers)]
        base = layers * experts
        gain_attn = [misc_all[base + l][None] for l in range(layers)]
        gain_mlp = [misc_all[base + layers + l][None] for l in range(layers)]
        gain_final = misc_all[base + 2 * layers][None]
        known_ints = known[:, n_misc : n_misc + ints.shape[0]].astype(I32)
        ids_all = known_ints[:, :toks]
        labels_all = known_ints[:, toks : 2 * toks]
        starts_all = known_ints[:, 2 * toks :].reshape(device_count, layers, experts + 1)

        attn_pack = jnp.concatenate([w_query, w_key, w_value, w_attn_out], axis=2).astype(BF16)
        attn_all = lax.all_gather(attn_pack, 'fsdp')
        attn_w = [attn_all[:, l].reshape(width, -1) for l in range(layers)]

        def gather(x):
            return lax.all_gather(x.astype(BF16), 'fsdp')

        expert_w = [(gather(m_gate[l]), gather(m_up[l]), gather(w_down[l])) for l in range(layers)]
        head_w = lax.all_gather(jnp.pad(m_head.astype(BF16), ((0, -vocab % (2 * TV)), (0, 0))), 'fsdp')

        partner_ids = lax.dynamic_index_in_dim(ids_all, pair * 2 + 1 - me, 0, keepdims=False)
        wanted = jnp.concatenate([tok_ids[0], partner_ids]) - me * vocab_share
        taken = jnp.take(embedding, jnp.clip(wanted, 0, vocab_share - 1), axis=0).astype(BF16)
        sent = lax.ppermute(taken[toks:], 'fsdp', swap)
        is_mine = (wanted[:toks] >= 0) & (wanted[:toks] < vocab_share)
        x = jnp.where(is_mine[:, None], taken[:toks], sent).astype(F32)

        cos_tab, sin_tab = rope_tables(tok_pos[0])
        attend = functools.partial(attention, cos_tab=cos_tab, sin_tab=sin_tab, q_width=q_width, kv_width=kv_width)

        attn_vjps, xs_all, kept = [], [], []
        for l in range(layers):
            x, attn_vjp = jax.vjp(attend, x, gain_attn[l], attn_w[l])
            attn_vjps.append(attn_vjp)
            pos, start = placed[l]
            out, xs, y0, y1 = moe_fwd(start, x, gain_mlp[l], w_r[l], pos.T, pos, experts_of[l], *expert_w[l], rows)
            kept.append((x, xs, y0, y1))
            xs_all.append(lax.all_gather(xs, both))
            x = out

        fin, lse, dx, d_final, loss = head(x, gain_final, tok_labels[0][:, None], head_w, vocab, tokens_all)
        fin_all = lax.all_gather(fin, both)

        extra = jnp.pad(lse.reshape(1, toks), ((0, 7), (0, width - toks)))
        dys_all = [None] * layers
        reduced = [None] * layers
        for l in reversed(range(layers)):
            x, xs, y0, y1 = kept[l]
            pos, start = placed[l]
            dx, dys, d_router, d_mlp = moe_bwd(start, dx, x, gain_mlp[l], w_r[l], pos.T, pos, experts_of[l].T, experts_of[l], y0, y1, xs, extra, *expert_w[l], rows)
            dys_all[l] = lax.all_gather(dys, both)
            dx, d_attn, d_w = attn_vjps[l](dx)
            tail = jnp.concatenate([d_router, d_attn.astype(F32), d_mlp, d_final, loss])
            tail = tail.reshape(-1, 2, half).swapaxes(0, 1).reshape(2, -1)
            wide = d_w.shape[1]
            tail = jnp.pad(tail, ((0, 0), (0, -tail.shape[1] % (8 * wide)))).reshape(2, -1, wide)
            local = jnp.concatenate([d_w.astype(F32).reshape(2, half, wide), tail], axis=1)
            reduced[l] = lax.psum(lax.psum_scatter(local, 'fsdp', scatter_dimension=0, tiled=False), 'rep')

        d_rows = lax.all_gather(dx.astype(BF16), both).reshape(tokens_all, width)

        lse_all = dys_all[layers - 1][:, rows : rows + 1, :toks]
        new_experts = None
        for l in reversed(range(layers)):
            new_experts = expert_dw(l, starts_all[:, l], fs, lr, xs_all[l], dys_all[l], *expert_w[l], m_gate, m_up, w_down, new_experts)
        new_head, other_grad = head_dw(fs, lr, fin_all, lse_all, labels_all[:, None], head_w, m_head, tokens_all)
        new_head = head_upd(fs, lr, lax.ppermute(other_grad, 'fsdp', swap), m_head, new_head)

        block = 1336
        local_id = ids_all.reshape(-1) - me * vocab_share
        key = jnp.where((local_id >= 0) & (local_id < vocab_share), local_id, vocab_share)
        keys, perm = lax.sort((key, lax.iota(I32, tokens_all)), num_keys=1)
        edges = jnp.arange(vocab_share // block + 1, dtype=I32) * block
        bounds = jnp.sum(key[None, :] < edges[:, None], axis=1).astype(I32)
        new_embedding = embed_upd(bounds, keys, perm, lr, d_rows, embedding, block)

        def update(master, pick):
            return master - learn_rate * jnp.stack([pick(reduced[l]) for l in range(layers)])

        def tail_of(r, first, count):
            return r[half:].reshape(-1)[first * half : (first + count) * half].reshape(count, half)

        v_at = q_width + kv_width
        new_query = update(w_query, lambda r: r[:half, :q_width])
        new_key = update(w_key, lambda r: r[:half, q_width:v_at])
        new_value = update(w_value, lambda r: r[:half, v_at : v_at + kv_width])
        new_attn_out = update(w_attn_out, lambda r: r[:half, v_at + kv_width :])
        new_router = update(w_router, lambda r: tail_of(r, 0, experts).T)
        new_g_attn = update(g_attn, lambda r: tail_of(r, experts, 1)[0])
        new_g_mlp = update(g_mlp, lambda r: tail_of(r, experts + 1, 1)[0])
        new_final = g_final - learn_rate * tail_of(reduced[0], experts + 2, 1)[0]
        both_loss = tail_of(reduced[0], experts + 3, 1)[0, 0]
        new_gate, new_up, new_down = new_experts
        return (new_embedding, new_query, new_key, new_value, new_attn_out, new_g_attn, new_g_mlp, new_router,
                jnp.swapaxes(new_gate, 2, 3), jnp.swapaxes(new_up, 2, 3), new_down, new_final, new_head.T, both_loss)

    return jax.shard_map(step, mesh=mesh, in_specs=in_specs, out_specs=out_specs, check_vma=False)
```

```python
import functools
import jax
import jax.numpy as jnp
from jax import lax
from jax.experimental import pallas as pl
from jax.experimental.pallas import tpu as pltpu
from jax.sharding import PartitionSpec as P

HEAD_DIM = 128
ROPE_THETA = 1000000.0
NORM_EPS = 1e-5
LOG2E = 1.4426950408889634
LN2 = 0.6931471805599453
F32 = jnp.float32
BF16 = jnp.bfloat16
I32 = jnp.int32
TILE = 16
HEAD_STEPS = 12
HEAD_PIECE = 512
DW_PIECE = 384
LSE_ROWS = 72
SUBLANES = 8
NEG = -1e30
ROW, COL = 0, 1


def contract(a, b, ca, cb):
    return lax.dot_general(a, b, (((ca,), (cb,)), ((), ())), preferred_element_type=F32)


def dot(a, b):
    return contract(a, b, COL, ROW)


def dot_nt(a, b):
    return contract(a, b, COL, COL)


def dot_tn(a, b):
    return contract(a, b, ROW, ROW)


def get(ref):
    return ref[...]


def put(ref, value):
    ref[...] = value


def fill(ref, value):
    put(ref, jnp.full(ref.shape, value, ref.dtype))


def iota(shape, axis):
    return lax.broadcasted_iota(I32, shape, axis)


def axis_sum(x, axis):
    return jnp.sum(x, axis=axis, keepdims=True)


def keep(mask, x):
    return jnp.where(mask, x, 0.0)


def hot(mask):
    return jnp.where(mask, 1.0, 0.0).astype(BF16)


def pair_of(x, axis):
    return jnp.split(x, 2, axis=axis)


def side_by_side(ref):
    return jnp.concatenate([ref[core].reshape(ref.shape[-2:]) for core in range(2)], axis=COL)


def rms_stats(x):
    return lax.rsqrt(jnp.mean(x * x, axis=-1, keepdims=True) + NORM_EPS)


def rms_norm(x, gain):
    return (x * rms_stats(x) * gain).astype(BF16)


def rms_norm_bwd(x, gain, d_normed):
    inv = rms_stats(x)
    unit = x * inv
    d_gain = axis_sum(d_normed * unit, ROW)
    d_unit = d_normed * gain
    d_x = inv * (d_unit - unit * jnp.mean(d_unit * unit, axis=-1, keepdims=True))
    return d_x, d_gain


def split3(x):
    hi = x.astype(BF16)
    rest = x - hi.astype(F32)
    mid = rest.astype(BF16)
    return hi, mid, (rest - mid.astype(F32)).astype(BF16)


def select_rows(onehot, x):
    hi, mid, lo = split3(x)
    return dot(onehot, hi) + dot(onehot, mid) + dot(onehot, lo)


def params(vmem_mib, **kw):
    return pltpu.CompilerParams(vmem_limit_bytes=vmem_mib << 20, **kw)


def whole(shape):
    zeros = (0,) * len(shape)
    return pl.BlockSpec(shape, lambda *_: zeros)


def route_masks(pos_row, rows):
    return [iota((rows, pos.shape[COL]), ROW) == pos for pos in pair_of(pos_row, ROW)]


def moe_fwd_kernel(off, x_ref, gain_ref, wr_ref, prow_ref, pcol_ref, ecol_ref, wg_ref, wu_ref, wd_ref,
                   out_ref, xs_out, y0_out, y1_out, xs_s, down_s, *, rows, blk):
    expert = pl.program_id(0)
    toks = x_ref.shape[0]

    @pl.when(expert == 0)
    def _():
        normed = rms_norm(get(x_ref), get(gain_ref))
        hit0, hit1 = route_masks(get(prow_ref), rows)
        spread = hot(hit0 | hit1)
        xs = dot(spread, normed).astype(BF16)
        put(xs_out, xs)
        xs_s[pl.ds(0, rows), :] = xs
        xs_s[pl.ds(rows, blk), :] = jnp.zeros((blk, xs.shape[1]), BF16)
        fill(down_s, 0)

    w_gate = side_by_side(wg_ref)
    w_up = side_by_side(wu_ref)
    w_down = get(wd_ref).reshape(w_gate.shape)
    start = off[expert]
    count = off[expert + 1] - start

    def body(i, carry):
        at = pl.multiple_of(start + i * blk, TILE)
        xs = xs_s[pl.ds(at, blk), :]
        gate = dot_nt(w_gate, xs)
        up = dot_nt(w_up, xs)
        hidden = (gate * jax.nn.sigmoid(gate) * up).astype(BF16)
        down_s[pl.ds(at, blk), :] = dot_tn(hidden, w_down)
        return carry

    lax.fori_loop(0, (count + blk - 1) // blk, body, 0)

    @pl.when(expert == pl.num_programs(0) - 1)
    def _():
        x = get(x_ref)
        normed = rms_norm(x, get(gain_ref))
        logits = dot_nt(normed, get(wr_ref))
        gate0, gate1 = pair_gates(logits, get(ecol_ref), COL)
        col_id = iota((toks, rows), COL)
        slot0, slot1 = pair_of(get(pcol_ref), COL)
        pick0 = hot(col_id == slot0)
        pick1 = hot(col_id == slot1)
        hi, mid, lo = split3(down_s[:rows])
        y0 = dot(pick0, hi) + dot(pick0, mid) + dot(pick0, lo)
        y1 = dot(pick1, hi) + dot(pick1, mid) + dot(pick1, lo)
        put(y0_out, y0)
        put(y1_out, y1)
        put(out_ref, x + (y0 * gate0 + y1 * gate1))


def pair_gates(logits, experts, axis):
    ids = iota(logits.shape, axis)
    r0, r1 = [axis_sum(keep(ids == chosen, logits), axis) for chosen in pair_of(experts, axis)]
    top = jnp.maximum(r0, r1)
    e0 = jnp.exp(r0 - top)
    e1 = jnp.exp(r1 - top)
    return e0 / (e0 + e1), e1 / (e0 + e1)


def moe_bwd_kernel(off, dx_ref, x_ref, gain_ref, wr_ref, prow_ref, pcol_ref, erow_ref, ecol_ref, y0_ref, y1_ref, xs_ref,
                   wg_ref, wu_ref, wd_ref, dx_out, dys_out, dwr_out, dg_out, xs_s, dys_s, dxs_s, *, rows, blk):
    expert = pl.program_id(0)
    toks, width = x_ref.shape

    @pl.when(expert == 0)
    def _():
        dx = get(dx_ref)
        normed = rms_norm(get(x_ref), get(gain_ref))
        logits_t = dot_nt(get(wr_ref), normed)
        gate0, gate1 = pair_gates(logits_t, get(erow_ref), ROW)
        hit0, hit1 = route_masks(get(prow_ref), rows)
        spread = hot(hit0 | hit1)
        gate_rows = axis_sum(keep(hit0, gate0) + keep(hit1, gate1), COL)
        dys = select_rows(spread, dx) * gate_rows
        put(dys_out, dys)
        dys_s[pl.ds(0, rows), :] = dys.astype(BF16)
        dys_s[pl.ds(rows, blk), :] = jnp.zeros((blk, width), BF16)
        xs_s[pl.ds(0, rows), :] = get(xs_ref)
        xs_s[pl.ds(rows, blk), :] = jnp.zeros((blk, width), BF16)
        fill(dxs_s, 0)

    w_gate = side_by_side(wg_ref)
    w_up = side_by_side(wu_ref)
    w_down = get(wd_ref).reshape(w_gate.shape)
    start = off[expert]
    count = off[expert + 1] - start

    def body(i, carry):
        at = pl.multiple_of(start + i * blk, TILE)
        xs = xs_s[pl.ds(at, blk), :]
        dys = dys_s[pl.ds(at, blk), :]
        gate = dot_nt(w_gate, xs)
        up = dot_nt(w_up, xs)
        d_hidden = dot_nt(w_down, dys)
        d_gate, d_up, _ = glu_bwd(gate, up, d_hidden)
        dxs_s[pl.ds(at, blk), :] = dot_tn(d_gate, w_gate) + dot_tn(d_up, w_up)
        return carry

    lax.fori_loop(0, (count + blk - 1) // blk, body, 0)

    @pl.when(expert == pl.num_programs(0) - 1)
    def _():
        x = get(x_ref)
        dx = get(dx_ref)
        gain = get(gain_ref)
        normed = rms_norm(x, gain)
        logits = dot_nt(normed, get(wr_ref))
        experts = get(ecol_ref)
        gate0, gate1 = pair_gates(logits, experts, COL)
        d_gate0 = axis_sum(dx * get(y0_ref), COL)
        d_gate1 = axis_sum(dx * get(y1_ref), COL)
        mean = gate0 * d_gate0 + gate1 * d_gate1
        first, second = pair_of(experts, COL)
        ids = iota(logits.shape, COL)
        d_logits = (keep(ids == first, gate0 * (d_gate0 - mean)) + keep(ids == second, gate1 * (d_gate1 - mean))).astype(BF16)
        put(dwr_out, dot_tn(d_logits, normed))
        col_id = iota((toks, rows), COL)
        slot0, slot1 = pair_of(get(pcol_ref), COL)
        collect = hot((col_id == slot0) | (col_id == slot1))
        d_normed = select_rows(collect, dxs_s[pl.ds(0, rows), :]) + dot(d_logits, get(wr_ref))
        d_x, d_gain = rms_norm_bwd(x, gain, d_normed.astype(BF16).astype(F32))
        put(dx_out, dx + d_x)
        put(dg_out, d_gain)


def glu_bwd(gate, up, d_hidden):
    sig = jax.nn.sigmoid(gate)
    act = gate * sig
    d_gate = (d_hidden * up * (sig + act * (1.0 - sig))).astype(BF16)
    d_up = (d_hidden * act).astype(BF16)
    return d_gate, d_up, act


def expert_specs(ff, half):
    up_spec = pl.BlockSpec((2, 1, ff, half), lambda e, *_: (0, e, 0, 0))
    down_spec = pl.BlockSpec((2, 1, ff // 2, 2 * half), lambda e, *_: (0, e, 0, 0))
    return [up_spec, up_spec, down_spec]


def moe_fwd(off, x, gain, w_r, pos_row, pos_col, exp_col, w_gate, w_up, w_down, rows):
    toks, width = x.shape
    experts, ff = w_gate.shape[1], w_gate.shape[2]
    blk = 128
    tok_out = jax.ShapeDtypeStruct((toks, width), F32)
    small = [x, gain, w_r, pos_row, pos_col, exp_col]
    return pl.pallas_call(
        functools.partial(moe_fwd_kernel, rows=rows, blk=blk),
        out_shape=(tok_out, jax.ShapeDtypeStruct((rows, width), BF16), tok_out, tok_out),
        grid_spec=pltpu.PrefetchScalarGridSpec(
            num_scalar_prefetch=1,
            grid=(experts,),
            in_specs=[whole(a.shape) for a in small] + expert_specs(ff, width // 2),
            out_specs=(whole((toks, width)), whole((rows, width)), whole((toks, width)), whole((toks, width))),
            scratch_shapes=[pltpu.VMEM((rows + blk, width), BF16), pltpu.VMEM((rows + blk, width), F32)],
        ),
        compiler_params=params(48),
        cost_estimate=pl.CostEstimate(flops=30_000_000_000, bytes_accessed=45_000_000, transcendentals=0),
        name="moe_fwd",
    )(off, *small, w_gate, w_up, w_down)


def moe_bwd(off, dx, x, gain, w_r, pos_row, pos_col, exp_row, exp_col, y0, y1, xs, w_gate, w_up, w_down, rows):
    toks, width = x.shape
    experts, ff = w_gate.shape[1], w_gate.shape[2]
    blk = 128
    small = [dx, x, gain, w_r, pos_row, pos_col, exp_row, exp_col, y0, y1, xs]
    out_shapes = (
        jax.ShapeDtypeStruct((toks, width), F32),
        jax.ShapeDtypeStruct((rows, width), F32),
        jax.ShapeDtypeStruct((experts, width), F32),
        jax.ShapeDtypeStruct((1, width), F32),
    )
    return pl.pallas_call(
        functools.partial(moe_bwd_kernel, rows=rows, blk=blk),
        out_shape=out_shapes,
        grid_spec=pltpu.PrefetchScalarGridSpec(
            num_scalar_prefetch=1,
            grid=(experts,),
            in_specs=[whole(a.shape) for a in small] + expert_specs(ff, width // 2),
            out_specs=tuple(whole(s.shape) for s in out_shapes),
            scratch_shapes=[
                pltpu.VMEM((rows + blk, width), BF16),
                pltpu.VMEM((rows + blk, width), BF16),
                pltpu.VMEM((rows + blk, width), F32),
            ],
        ),
        compiler_params=params(60),
        cost_estimate=pl.CostEstimate(flops=50_000_000_000, bytes_accessed=50_000_000, transcendentals=0),
        name="moe_bwd",
    )(off, *small, w_gate, w_up, w_down)


def expert_dw_kernel(off, fs, lr_ref, xs_hbm, dys_hbm, wg_ref, wu_ref, wd_ref, mg_ref, mu_ref, md_ref, *refs, blk, alias):
    refs = refs[3:] if alias else refs
    og_ref, ou_ref, od_ref, xbuf, dbuf, sems, acc_g, acc_u, acc_d = refs
    expert = pl.program_id(0)
    experts = pl.num_programs(0)
    seqs = xs_hbm.shape[0]
    ff, half = acc_g.shape
    mine = fs[0]

    def copies(e, slot, go):
        at = 0
        for s in range(seqs):
            start = pl.multiple_of(off[s, e], TILE)
            count = pl.multiple_of(off[s, e + 1] - off[s, e], TILE)
            dst = pl.multiple_of(at, TILE)

            @pl.when(count > 0)
            def _():
                for hbm, buf, k in ((xs_hbm, xbuf, 0), (dys_hbm, dbuf, 1)):
                    copy = pltpu.make_async_copy(hbm.at[s, pl.ds(start, count), :], buf.at[slot, pl.ds(dst, count), :], sems.at[slot, k])
                    if go:
                        copy.start()
                    else:
                        copy.wait()

            at = at + count
        return at

    slot = lax.rem(expert, 2)

    @pl.when(expert == 0)
    def _():
        copies(0, 0, True)

    @pl.when(expert + 1 < experts)
    def _():
        copies(expert + 1, 1 - slot, True)

    total = pl.multiple_of(copies(expert, slot, False), TILE)
    xbuf[slot, pl.ds(total, blk), :] = jnp.zeros((blk, xbuf.shape[2]), BF16)
    dbuf[slot, pl.ds(total, blk), :] = jnp.zeros((blk, dbuf.shape[2]), F32)
    fill(acc_g, 0)
    fill(acc_u, 0)
    fill(acc_d, 0)
    w_gate = side_by_side(wg_ref)
    w_up = side_by_side(wu_ref)
    w_down = get(wd_ref).reshape(w_gate.shape)

    def body(i, carry):
        at = pl.multiple_of(i * blk, blk)
        xs = xbuf[slot, pl.ds(at, blk), :]
        own = xbuf[slot, pl.ds(at, blk), pl.ds(pl.multiple_of(mine * half, half), half)]
        dys = dbuf[slot, pl.ds(at, blk), :].astype(BF16)
        gate = dot_nt(w_gate, xs)
        up = dot_nt(w_up, xs)
        d_hidden = dot_nt(w_down, dys)
        d_gate, d_up, act = glu_bwd(gate, up, d_hidden)
        hidden = (act * up).astype(BF16)
        put(acc_g, get(acc_g) + dot(d_gate, own))
        put(acc_u, get(acc_u) + dot(d_up, own))
        hidden_own = jnp.where(mine == 0, hidden[: ff // 2], hidden[ff // 2 :])
        put(acc_d, get(acc_d) + dot(hidden_own, dys))
        return carry

    lax.fori_loop(0, (total + blk - 1) // blk, body, 0)
    for out, master, acc in ((og_ref, mg_ref, acc_g), (ou_ref, mu_ref, acc_u), (od_ref, md_ref, acc_d)):
        put(out, get(master) - get(lr_ref) * get(acc).reshape(out.shape))


def expert_dw(layer, off, fs, lr, xs, dys, w_gate, w_up, w_down, m_gate, m_up, m_down, prev):
    seqs, _, width = xs.shape
    _, experts, ff, half = m_gate.shape
    blk = 256
    most = seqs * ((width + TILE - 1) // TILE * TILE)
    any_spec = pl.BlockSpec(memory_space=pl.ANY)
    up_master = pl.BlockSpec((1, 1, ff, half), lambda e, *_: (layer, e, 0, 0))
    down_master = pl.BlockSpec((1, 1, ff // 2, width), lambda e, *_: (layer, e, 0, 0))
    masters = [up_master, up_master, down_master]
    alias = prev is not None
    in_specs = [whole(lr.shape), any_spec, any_spec] + expert_specs(ff, half) + masters
    in_specs += [any_spec] * 3 if alias else []
    return pl.pallas_call(
        functools.partial(expert_dw_kernel, blk=blk, alias=alias),
        out_shape=tuple(jax.ShapeDtypeStruct(m.shape, F32) for m in (m_gate, m_up, m_down)),
        grid_spec=pltpu.PrefetchScalarGridSpec(
            num_scalar_prefetch=2,
            grid=(experts,),
            in_specs=in_specs,
            out_specs=tuple(masters),
            scratch_shapes=[
                pltpu.VMEM((2, most + blk, width), BF16),
                pltpu.VMEM((2, most + blk, width), F32),
                pltpu.SemaphoreType.DMA((2, 2)),
                pltpu.VMEM((ff, half), F32),
                pltpu.VMEM((ff, half), F32),
                pltpu.VMEM((ff // 2, width), F32),
            ],
        ),
        input_output_aliases={11: 0, 12: 1, 13: 2} if alias else {},
        compiler_params=params(62),
        cost_estimate=pl.CostEstimate(flops=90_000_000_000, bytes_accessed=150_000_000, transcendentals=0),
        name="expert_dw",
    )(off, fs, lr, xs, dys, w_gate, w_up, w_down, m_gate, m_up, m_down, *(prev or ()))


def pieces(total, size):
    edges = [*range(0, total, size), total]
    return list(zip(edges, edges[1:]))


def staggered(items, first, second):
    held = None
    for item in items:
        made = first(item)
        if held is not None:
            second(*held)
        held = (item, made)
    second(*held)


def own_first(x, mine):
    lower, upper = pair_of(x, COL)
    return jnp.where(mine == 0, x, jnp.concatenate([upper, lower], axis=COL))


def sublane_groups(x):
    return x.reshape(-1, SUBLANES, x.shape[COL])


def both_cores(refs, lo, hi):
    return jnp.concatenate([ref[lo:hi] for ref in refs], axis=COL)


def head_kernel(fs, x_ref, gain_ref, lab_ref, wa_ref, wb_ref, fin_out, lse_out, dx_out, dg_out, loss_out, fin_s, top_s, sum_s, pick_s, acc_s, *, tokens_all):
    sweep = pl.program_id(0)
    step = pl.program_id(1)
    last = pl.num_programs(1) - 1
    tile = wa_ref.shape[ROW]
    mine = fs[0]
    parts = pieces(tile, HEAD_PIECE)

    @pl.when((sweep == 0) & (step == 0))
    def _():
        fin = rms_norm(get(x_ref), get(gain_ref))
        put(fin_out, fin)
        put(fin_s, own_first(fin, mine).T)
        fill(top_s, NEG)
        fill(sum_s, 0)
        fill(pick_s, 0)
        fill(acc_s, 0)

    def logits_of(part):
        return dot(both_cores((wa_ref, wb_ref), *part), get(fin_s)) * LOG2E

    def take_sums(part, logits):
        grouped = sublane_groups(logits)
        old = get(top_s)
        new = jnp.maximum(old, jnp.max(grouped, axis=ROW))
        put(sum_s, get(sum_s) * jnp.exp2(old - new) + jnp.sum(jnp.exp2(grouped - new), axis=ROW))
        put(top_s, new)

    @pl.when(sweep == 0)
    def _():
        staggered(parts, logits_of, take_sums)

    @pl.when((sweep == 0) & (step == last))
    def _():
        top = jnp.max(get(top_s), axis=ROW, keepdims=True)
        total = axis_sum(get(sum_s) * jnp.exp2(get(top_s) - top), ROW)
        put(lse_out, jnp.broadcast_to(top + jnp.log2(total), lse_out.shape))

    def gradient(part):
        logits = logits_of(part)
        prob = jnp.exp2(logits - (lse_out[:1] + jnp.log2(jnp.float32(tokens_all))))
        hit = iota(logits.shape, ROW) == get(lab_ref) - (step * tile + part[0])
        put(pick_s, get(pick_s) + jnp.sum(sublane_groups(keep(hit, logits)), axis=ROW))
        return (prob - jnp.where(hit, 1.0 / tokens_all, 0.0)).astype(BF16)

    def add_gradient(part, grad):
        put(acc_s, get(acc_s) + dot_tn(grad, both_cores((wa_ref, wb_ref), *part)))

    @pl.when(sweep == 1)
    def _():
        staggered(parts, gradient, add_gradient)

    @pl.when((sweep == 1) & (step == last))
    def _():
        per_tok = (lse_out[:1] - axis_sum(get(pick_s), ROW)) * (LN2 / tokens_all)
        put(loss_out, jnp.broadcast_to(axis_sum(per_tok, COL), loss_out.shape))
        d_fin = own_first(get(acc_s), mine).astype(BF16).astype(F32)
        d_x, d_gain = rms_norm_bwd(get(x_ref), get(gain_ref), d_fin)
        put(dx_out, d_x)
        put(dg_out, d_gain)


def head(fs, x, gain, labels, w_own, w_other, tokens_all):
    toks, width = x.shape
    vocab, half = w_own.shape
    tile = vocab // HEAD_STEPS
    out_shapes = (
        jax.ShapeDtypeStruct((toks, width), BF16),
        jax.ShapeDtypeStruct((LSE_ROWS, toks), F32),
        jax.ShapeDtypeStruct((toks, width), F32),
        jax.ShapeDtypeStruct((1, width), F32),
        jax.ShapeDtypeStruct((1, width), F32),
    )
    small = [x, gain, labels]
    w_spec = pl.BlockSpec((tile, half), lambda p, i, *_: (i, 0))
    return pl.pallas_call(
        functools.partial(head_kernel, tokens_all=tokens_all),
        out_shape=out_shapes,
        grid_spec=pltpu.PrefetchScalarGridSpec(
            num_scalar_prefetch=1,
            grid=(2, HEAD_STEPS),
            in_specs=[whole(a.shape) for a in small] + [w_spec, w_spec],
            out_specs=tuple(whole(s.shape) for s in out_shapes),
            scratch_shapes=[pltpu.VMEM((width, toks), BF16)] + [pltpu.VMEM((SUBLANES, toks), F32)] * 3 + [pltpu.VMEM((toks, width), F32)],
        ),
        compiler_params=params(56),
        cost_estimate=pl.CostEstimate(flops=55_000_000_000, bytes_accessed=70_000_000, transcendentals=0),
        name="head_own",
    )(fs, *small, w_own, w_other)


def head_dw_kernel(fs, fin_ref, lse_ref, lab_ref, wa_ref, wb_ref, own_out, oth_out, fin_s, fin_t, *, tokens_all):
    tile, half = wa_ref.shape
    seqs = fin_s.shape[0]
    mine = fs[0]
    base = (fs[1] * pl.num_programs(0) + pl.program_id(0)) * tile
    parts = pieces(tile, DW_PIECE)
    fill(own_out, 0)
    fill(oth_out, 0)

    @pl.when(pl.program_id(0) == 0)
    def _():
        for s in range(seqs):
            fin = own_first(fin_ref[mine * seqs + s], mine)
            fin_s[s] = fin
            fin_t[s] = fin.T

    def body(s, carry):
        lse = lse_ref[mine * seqs + s, :1] + jnp.log2(jnp.float32(tokens_all))
        lab = lab_ref[mine * seqs + s] - base

        def gradient(part):
            logits = dot(both_cores((wa_ref, wb_ref), *part), fin_t[s]) * LOG2E
            hit = iota(logits.shape, ROW) == lab - part[0]
            return (jnp.exp2(logits - lse) - jnp.where(hit, 1.0 / tokens_all, 0.0)).astype(BF16)

        def add_gradient(part, grad):
            rows = slice(*part)
            own_out[rows] += dot(grad, fin_s[s, :, :half])
            oth_out[rows] += dot(grad, fin_s[s, :, half:])

        staggered(parts, gradient, add_gradient)
        return carry

    lax.fori_loop(0, seqs, body, 0)


def head_dw(fs, fin, lse, labels, w_own, w_other, tokens_all):
    seqs, toks, width = fin.shape
    vocab, half = w_own.shape
    tile = vocab // HEAD_STEPS
    steps = HEAD_STEPS // (seqs // 2)
    out = jax.ShapeDtypeStruct((steps * tile, half), F32)
    out_spec = pl.BlockSpec((tile, half), lambda i, *_: (i, 0))
    w_spec = pl.BlockSpec((tile, half), lambda i, f: (f[1] * steps + i, 0))
    return pl.pallas_call(
        functools.partial(head_dw_kernel, tokens_all=tokens_all),
        out_shape=(out, out),
        grid_spec=pltpu.PrefetchScalarGridSpec(
            num_scalar_prefetch=1,
            grid=(steps,),
            in_specs=[whole(fin.shape), whole(lse.shape), whole(labels.shape), w_spec, w_spec],
            out_specs=(out_spec, out_spec),
            scratch_shapes=[pltpu.VMEM((seqs // 2, toks, width), BF16), pltpu.VMEM((seqs // 2, width, toks), BF16)],
        ),
        compiler_params=params(56),
        cost_estimate=pl.CostEstimate(flops=40_000_000_000, bytes_accessed=40_000_000, transcendentals=0),
        name="head_dw",
    )(fs, fin, lse, labels, w_own, w_other)


def head_upd_kernel(fs, lr_ref, own_ref, recv_ref, m_ref, new_out):
    put(new_out, get(m_ref) - get(lr_ref) * (get(own_ref) + get(recv_ref)))


def head_upd(fs, lr, own, received, master):
    rows, half = own.shape
    tile = master.shape[ROW] // HEAD_STEPS
    steps = rows // tile
    spec = pl.BlockSpec((tile, half), lambda i, *_: (i, 0))
    return pl.pallas_call(
        head_upd_kernel,
        out_shape=jax.ShapeDtypeStruct((rows, half), F32),
        grid_spec=pltpu.PrefetchScalarGridSpec(
            num_scalar_prefetch=1,
            grid=(steps,),
            in_specs=[whole(lr.shape), spec, spec, pl.BlockSpec((tile, half), lambda i, f: (f[1] * steps + i, 0))],
            out_specs=spec,
        ),
        compiler_params=params(48),
        cost_estimate=pl.CostEstimate(flops=8_000_000_000, bytes_accessed=33_000_000, transcendentals=0),
        name="head_upd",
    )(fs, lr, own, received, master)


def embed_upd_kernel(bounds, keys, perm, lr_ref, rows_ref, m_ref, new_out, wide_s):
    step = pl.program_id(0)
    rows = m_ref.shape[0]

    @pl.when(step == 0)
    def _():
        put(wide_s, get(rows_ref).astype(F32) * get(lr_ref))

    put(new_out, get(m_ref))

    def body(j, carry):
        at = new_out.at[pl.ds(keys[j] - step * rows, 1)]
        put(at, get(at) - get(wide_s.at[pl.ds(perm[j], 1)]))
        return carry

    lax.fori_loop(bounds[step], bounds[step + 1], body, 0)


def embed_upd(bounds, keys, perm, lr, grads, master, rows):
    vocab, width = master.shape
    return pl.pallas_call(
        embed_upd_kernel,
        out_shape=jax.ShapeDtypeStruct((vocab, width), F32),
        grid_spec=pltpu.PrefetchScalarGridSpec(
            num_scalar_prefetch=3,
            grid=(vocab // rows,),
            in_specs=[
                whole(lr.shape),
                whole(grads.shape),
                pl.BlockSpec((rows, width), lambda i, *_: (i, 0)),
            ],
            out_specs=pl.BlockSpec((rows, width), lambda i, *_: (i, 0)),
            scratch_shapes=[pltpu.VMEM(grads.shape, F32)],
        ),
        compiler_params=params(48),
        cost_estimate=pl.CostEstimate(flops=25_000_000_000, bytes_accessed=66_000_000, transcendentals=0),
        name="embed_upd",
    )(bounds, keys, perm, lr, grads, master)


def rope_tables(positions):
    inv_freq = ROPE_THETA ** (-jnp.arange(0, HEAD_DIM, 2, dtype=F32) / HEAD_DIM)
    angle = positions.astype(F32)[:, None] * inv_freq
    cos, sin = jnp.cos(angle), jnp.sin(angle)
    return jnp.concatenate([cos, cos], axis=COL), jnp.concatenate([-sin, sin], axis=COL)


def half_turn(x):
    return pltpu.roll(x, HEAD_DIM // 2, COL)


def rope(x, cos, sin):
    return x * cos + half_turn(x) * sin


def rope_bwd(dx, cos, sin):
    return dx * cos + half_turn(dx * sin)


def qkv_heads(x, gain, weights, cos, sin, q_width):
    normed = rms_norm(x, gain)
    all_heads = jnp.split(dot(normed, weights), weights.shape[COL] // HEAD_DIM, axis=COL)
    count = q_width // HEAD_DIM
    queries = [rope(q, cos, sin).astype(BF16) for q in all_heads[:count]]
    key, value = all_heads[count:]
    return normed, queries, rope(key, cos, sin).astype(BF16), value.astype(BF16)


def attn_probs(query, key):
    scores = dot_nt(query, key) * HEAD_DIM ** -0.5
    scores = jnp.where(iota(scores.shape, ROW) >= iota(scores.shape, COL), scores, NEG)
    raised = jnp.exp(scores - jnp.max(scores, axis=COL, keepdims=True))
    return raised / axis_sum(raised, COL)


def attn_fwd_kernel(x_ref, gain_ref, cos_ref, sin_ref, w_ref, out_ref, *, q_width, in_width):
    x = get(x_ref)
    weights = get(w_ref).reshape(x.shape[COL], -1)
    _, queries, key, value = qkv_heads(x, get(gain_ref), weights[:, :in_width], get(cos_ref), get(sin_ref), q_width)
    mixed = [dot(attn_probs(query, key).astype(BF16), value).astype(BF16) for query in queries]
    put(out_ref, x + dot(jnp.concatenate(mixed, axis=COL), weights[:, in_width:]))


def attn_bwd_kernel(dx_ref, x_ref, gain_ref, cos_ref, sin_ref, dwr_ref, dgm_ref, dgf_ref, loss_ref, w_ref, dx_out, dw_out, *, q_width, in_width):
    x = get(x_ref)
    d_out = get(dx_ref)
    gain, cos, sin = get(gain_ref), get(cos_ref), get(sin_ref)
    weights = get(w_ref).reshape(x.shape[COL], -1)
    half = x.shape[COL] // 2
    normed, queries, key, value = qkv_heads(x, gain, weights[:, :in_width], cos, sin, q_width)
    d_proj = d_out.astype(BF16)
    d_mixed = jnp.split(dot_nt(d_proj, weights[:, in_width:]).astype(BF16), len(queries), axis=COL)
    mixed, d_heads = [], []
    d_key = d_value = None
    for query, d_mix in zip(queries, d_mixed):
        probs = attn_probs(query, key)
        rounded = probs.astype(BF16)
        mixed.append(dot(rounded, value).astype(BF16))
        d_probs = dot_nt(d_mix, value)
        d_scores = (probs * (d_probs - axis_sum(d_probs * probs, COL)) * HEAD_DIM ** -0.5).astype(BF16)
        d_heads.append(rope_bwd(dot(d_scores, key), cos, sin).astype(BF16))
        more_key, more_value = dot_tn(d_scores, query), dot_tn(rounded, d_mix)
        d_key = more_key if d_key is None else d_key + more_key
        d_value = more_value if d_value is None else d_value + more_value
    d_heads += [rope_bwd(d_key, cos, sin).astype(BF16), d_value.astype(BF16)]
    d_in = jnp.concatenate(d_heads, axis=COL)
    d_weights = jnp.concatenate([dot_tn(normed, d_in), dot_tn(jnp.concatenate(mixed, axis=COL), d_proj)], axis=COL)
    d_x, d_gain = rms_norm_bwd(x, gain, dot_nt(d_in, weights[:, :in_width]).astype(BF16).astype(F32))
    put(dx_out, d_out + d_x)
    for core, d_half in enumerate(pair_of(d_weights, ROW)):
        dw_out[core, :half] = d_half
    small = jnp.concatenate([get(dwr_ref), d_gain, get(dgm_ref), get(dgf_ref), get(loss_ref)], axis=ROW)
    per_row = d_weights.shape[COL] // half
    for i in range(small.shape[ROW]):
        row, at = half + i // per_row, i % per_row * half
        for core, part in enumerate(pair_of(small[i : i + 1], COL)):
            dw_out[core, row : row + 1, at : at + half] = part


def attn_specs(arrays, w_all, layer):
    spec = pl.BlockSpec((2, 1, *w_all.shape[2:]), lambda i: (0, layer, 0, 0))
    return [whole(a.shape) for a in arrays] + [spec]


def attn_fwd(layer, x, gain, cos, sin, w_all, q_width, in_width):
    small = [x, gain, cos, sin]
    return pl.pallas_call(
        functools.partial(attn_fwd_kernel, q_width=q_width, in_width=in_width),
        out_shape=jax.ShapeDtypeStruct(x.shape, F32),
        grid=(1,),
        in_specs=attn_specs(small, w_all, layer),
        out_specs=whole(x.shape),
        compiler_params=params(48),
        cost_estimate=pl.CostEstimate(flops=8_000_000_000, bytes_accessed=5_000_000, transcendentals=0),
        name="attn_fwd",
    )(*small, w_all)


def attn_bwd(layer, dx, x, gain, cos, sin, d_router, d_mlp, d_final, loss, w_all, q_width, in_width):
    small = [dx, x, gain, cos, sin, d_router, d_mlp, d_final, loss]
    half, wide = w_all.shape[2:]
    tail = -(-(d_router.shape[ROW] + 4) // (wide // half) // SUBLANES) * SUBLANES
    grads = jax.ShapeDtypeStruct((2, half + tail, wide), F32)
    return pl.pallas_call(
        functools.partial(attn_bwd_kernel, q_width=q_width, in_width=in_width),
        out_shape=(jax.ShapeDtypeStruct(x.shape, F32), grads),
        grid=(1,),
        in_specs=attn_specs(small, w_all, layer),
        out_specs=(whole(x.shape), whole(grads.shape)),
        compiler_params=params(60),
        cost_estimate=pl.CostEstimate(flops=15_000_000_000, bytes_accessed=10_000_000, transcendentals=0),
        name="attn_bwd",
    )(*small, w_all)


def routing(experts_of, experts):
    toks = experts_of.shape[0]
    hot = (experts_of[:, :, None] == jnp.arange(experts, dtype=I32)).astype(F32)
    both = hot[:, 0] + hot[:, 1]
    before = iota((toks, toks), 0) > iota((toks, toks), 1)
    ahead = dot(before.astype(BF16), both.astype(BF16))
    counts = jnp.sum(both, axis=0).astype(I32)
    padded = (counts + TILE - 1) // TILE * TILE
    upto = iota((experts + 1, experts), 0) > iota((experts + 1, experts), 1)
    starts = jnp.sum(jnp.where(upto, padded[None, :], 0), axis=1)
    place = starts[:experts].astype(F32) + ahead
    return jnp.sum(hot * place[:, None, :], axis=2).astype(I32), starts


def solution(mesh):
    device_count = mesh.shape['rep'] * mesh.shape['fsdp']
    both = ('rep', 'fsdp')
    batch_spec = P(both)
    layer_spec = P(None, 'fsdp')
    expert_spec = P(None, None, 'fsdp')
    param_specs = (P('fsdp'), layer_spec, layer_spec, layer_spec, layer_spec, layer_spec, layer_spec, layer_spec, expert_spec, expert_spec, expert_spec, P('fsdp'), P('fsdp'))
    in_specs = (batch_spec, batch_spec, batch_spec, P(None, both), P()) + param_specs
    out_specs = param_specs + (P(),)

    def step(tok_ids, tok_labels, tok_pos, expert_idx, learn_rate, embedding, w_query, w_key, w_value, w_attn_out, g_attn, g_mlp, w_router, w_gate, w_up, w_down, g_final, w_head):
        layers, half, q_width = w_query.shape
        kv_width = w_key.shape[2]
        width = 2 * half
        toks = tok_ids.shape[1]
        experts = w_router.shape[2]
        tokens_all = toks * device_count
        vocab_share = embedding.shape[0]
        rows = 2 * toks + experts * TILE
        me = lax.axis_index('fsdp')
        pair = lax.axis_index('rep')
        fs = jnp.stack([me, pair]).astype(I32)
        lr = learn_rate.reshape(1, 1)
        swap = [(0, 1), (1, 0)]

        m_gate = jnp.swapaxes(w_gate, 2, 3)
        m_up = jnp.swapaxes(w_up, 2, 3)
        m_head = w_head.T

        experts_of = expert_idx[:, 0]
        placed = [routing(experts_of[l], experts) for l in range(layers)]
        starts = jnp.stack([s for _, s in placed])
        ints = jnp.concatenate([tok_ids[0], tok_labels[0], starts.reshape(-1)]).astype(F32)
        misc = jnp.concatenate([jnp.swapaxes(w_router, 1, 2).reshape(layers * experts, half), g_attn, g_mlp, g_final[None]])
        misc = misc.astype(BF16).astype(F32).reshape(-1)
        packed = jnp.concatenate([misc, ints])
        n_misc = misc.shape[0]
        packed = jnp.pad(packed, (0, -packed.shape[0] % 1024)).reshape(-1, 128)
        known = lax.all_gather(packed, both).reshape(device_count, -1)
        two = lax.dynamic_slice_in_dim(known, pair * 2, 2, 0)[:, :n_misc].reshape(2, -1, half)
        misc_all = jnp.concatenate([two[0], two[1]], axis=1)
        w_r = [misc_all[l * experts : (l + 1) * experts].astype(BF16) for l in range(layers)]
        base = layers * experts
        gain_attn = [misc_all[base + l][None] for l in range(layers)]
        gain_mlp = [misc_all[base + layers + l][None] for l in range(layers)]
        gain_final = misc_all[base + 2 * layers][None]
        known_ints = known[:, n_misc : n_misc + ints.shape[0]].astype(I32)
        ids_all = known_ints[:, :toks]
        labels_all = known_ints[:, toks : 2 * toks]
        starts_all = known_ints[:, 2 * toks :].reshape(device_count, layers, experts + 1)

        attn_pack = jnp.concatenate([w_query, w_key, w_value, w_attn_out], axis=2).astype(BF16)
        attn_all = lax.all_gather(attn_pack, 'fsdp')

        def gather(x):
            return lax.all_gather(x.astype(BF16), 'fsdp')

        expert_w = [(gather(m_gate[l]), gather(m_up[l]), gather(w_down[l])) for l in range(layers)]
        head_w = (m_head.astype(BF16),)
        head_w += (lax.ppermute(head_w[0], 'fsdp', swap),)

        partner_ids = lax.dynamic_index_in_dim(ids_all, pair * 2 + 1 - me, 0, keepdims=False)
        wanted = jnp.concatenate([tok_ids[0], partner_ids]) - me * vocab_share
        taken = jnp.take(embedding, jnp.clip(wanted, 0, vocab_share - 1), axis=0).astype(BF16)
        sent = lax.ppermute(taken[toks:], 'fsdp', swap)
        is_mine = (wanted[:toks] >= 0) & (wanted[:toks] < vocab_share)
        x = jnp.where(is_mine[:, None], taken[:toks], sent).astype(F32)

        tables = rope_tables(tok_pos[0])
        widths = (q_width, q_width + 2 * kv_width)

        xs_all, kept = [], []
        for l in range(layers):
            mid = attn_fwd(l, x, gain_attn[l], *tables, attn_all, *widths)
            pos, start = placed[l]
            out, xs, y0, y1 = moe_fwd(start, mid, gain_mlp[l], w_r[l], pos.T, pos, experts_of[l], *expert_w[l], rows)
            kept.append((x, mid, xs, y0, y1))
            xs_all.append(lax.all_gather(xs, both))
            x = out

        fin, lse, dx, d_final, loss = head(fs, x, gain_final, tok_labels, *head_w, tokens_all)
        fin_all = lax.all_gather(fin, both)
        lse_all = lax.all_gather(lse, both)

        dys_all = [None] * layers
        reduced = [None] * layers
        new_head = None
        for l in reversed(range(layers)):
            x, mid, xs, y0, y1 = kept[l]
            pos, start = placed[l]
            dx, dys, d_router, d_mlp = moe_bwd(start, dx, mid, gain_mlp[l], w_r[l], pos.T, pos, experts_of[l].T, experts_of[l], y0, y1, xs, *expert_w[l], rows)
            dys_all[l] = lax.all_gather(dys, both)
            if new_head is None:
                fin_all, _ = lax.optimization_barrier((fin_all, dx))
                own_grad, other_grad = head_dw(fs, fin_all, lse_all, labels_all[:, None], *head_w, tokens_all)
                dx, _ = lax.optimization_barrier((dx, own_grad))
            dx, grads = attn_bwd(l, dx, x, gain_attn[l], *tables, d_router, d_mlp, d_final, loss, attn_all, *widths)
            if new_head is None:
                quarter = head_upd(fs, lr, own_grad, lax.ppermute(other_grad, 'fsdp', swap), m_head)
                new_head = lax.all_gather(quarter, 'rep', tiled=True)
            reduced[l] = lax.psum(lax.psum_scatter(grads, 'fsdp', scatter_dimension=0, tiled=False), 'rep')

        d_rows = lax.all_gather(dx.astype(BF16), both).reshape(tokens_all, width)

        new_experts = None
        for l in reversed(range(layers)):
            new_experts = expert_dw(l, starts_all[:, l], fs, lr, xs_all[l], dys_all[l], *expert_w[l], m_gate, m_up, w_down, new_experts)

        block = 1336
        local_id = ids_all.reshape(-1) - me * vocab_share
        key = jnp.where((local_id >= 0) & (local_id < vocab_share), local_id, vocab_share)
        keys, perm = lax.sort((key, lax.iota(I32, tokens_all)), num_keys=1)
        edges = jnp.arange(vocab_share // block + 1, dtype=I32) * block
        bounds = jnp.sum(key[None, :] < edges[:, None], axis=1).astype(I32)
        new_embedding = embed_upd(bounds, keys, perm, lr, d_rows, embedding, block)

        def update(master, pick):
            return master - learn_rate * jnp.stack([pick(reduced[l]) for l in range(layers)])

        def tail_of(r, first, count):
            return r[half:].reshape(-1)[first * half : (first + count) * half].reshape(count, half)

        v_at = q_width + kv_width
        new_query = update(w_query, lambda r: r[:half, :q_width])
        new_key = update(w_key, lambda r: r[:half, q_width:v_at])
        new_value = update(w_value, lambda r: r[:half, v_at : v_at + kv_width])
        new_attn_out = update(w_attn_out, lambda r: r[:half, v_at + kv_width :])
        new_router = update(w_router, lambda r: tail_of(r, 0, experts).T)
        new_g_attn = update(g_attn, lambda r: tail_of(r, experts, 1)[0])
        new_g_mlp = update(g_mlp, lambda r: tail_of(r, experts + 1, 1)[0])
        new_final = g_final - learn_rate * tail_of(reduced[0], experts + 2, 1)[0]
        both_loss = tail_of(reduced[0], experts + 3, 1)[0, 0]
        new_gate, new_up, new_down = new_experts
        return (new_embedding, new_query, new_key, new_value, new_attn_out, new_g_attn, new_g_mlp, new_router,
                jnp.swapaxes(new_gate, 2, 3), jnp.swapaxes(new_up, 2, 3), new_down, new_final, new_head.T, both_loss)

    return jax.shard_map(step, mesh=mesh, in_specs=in_specs, out_specs=out_specs, check_vma=False)
```

```python
import functools
import jax
import jax.numpy as jnp
from jax import lax
from jax.experimental import pallas as pl
from jax.experimental.pallas import tpu as pltpu
from jax.sharding import PartitionSpec as P

HEAD_DIM = 128
ROPE_THETA = 1000000.0
NORM_EPS = 1e-5
LOG2E = 1.4426950408889634
LN2 = 0.6931471805599453
F32 = jnp.float32
BF16 = jnp.bfloat16
I32 = jnp.int32
TILE = 16
HEAD_STEPS = 12
HEAD_PIECE = 512
DW_PIECE = 384
LSE_ROWS = 72
KNOWN = 40960
SUBLANES = 8
NEG = -1e30
ROW, COL = 0, 1
LANES = 128


def contract(a, b, ca, cb):
    return lax.dot_general(a, b, (((ca,), (cb,)), ((), ())), preferred_element_type=F32)


def dot(a, b):
    return contract(a, b, COL, ROW)


def dot_nt(a, b):
    return contract(a, b, COL, COL)


def dot_tn(a, b):
    return contract(a, b, ROW, ROW)


def get(ref):
    return ref[...]


def put(ref, value):
    ref[...] = value


def fill(ref, value):
    put(ref, jnp.full(ref.shape, value, ref.dtype))


def iota(shape, axis):
    return lax.broadcasted_iota(I32, shape, axis)


def axis_sum(x, axis):
    return jnp.sum(x, axis=axis, keepdims=True)


def keep(mask, x):
    return jnp.where(mask, x, 0.0)


def hot(mask):
    return jnp.where(mask, 1.0, 0.0).astype(BF16)


def pair_of(x, axis):
    return jnp.split(x, 2, axis=axis)


def rms_stats(x):
    return lax.rsqrt(jnp.mean(x * x, axis=-1, keepdims=True) + NORM_EPS)


def rms_norm(x, gain):
    return (x * rms_stats(x) * gain).astype(BF16)


def rms_norm_bwd(x, gain, d_normed):
    inv = rms_stats(x)
    unit = x * inv
    d_gain = axis_sum(d_normed * unit, ROW)
    d_unit = d_normed * gain
    d_x = inv * (d_unit - unit * jnp.mean(d_unit * unit, axis=-1, keepdims=True))
    return d_x, d_gain


def split3(x):
    hi = x.astype(BF16)
    rest = x - hi.astype(F32)
    mid = rest.astype(BF16)
    return hi, mid, (rest - mid.astype(F32)).astype(BF16)


def select_rows(onehot, x):
    hi, mid, lo = split3(x)
    return dot(onehot, hi) + dot(onehot, mid) + dot(onehot, lo)


def pieces(total, size):
    edges = [*range(0, total, size), total]
    return list(zip(edges, edges[1:]))


def staggered(items, first, second):
    held = None
    for item in items:
        made = first(item)
        if held is not None:
            second(*held)
        held = (item, made)
    second(*held)


def own_first(x, mine):
    lower, upper = pair_of(x, COL)
    return jnp.where(mine == 0, x, jnp.concatenate([upper, lower], axis=COL))


def sublane_groups(x):
    return x.reshape(-1, SUBLANES, x.shape[COL])


def both_cores(refs, lo, hi):
    return jnp.concatenate([ref[lo:hi] for ref in refs], axis=COL)


def params(vmem_mib, **kw):
    return pltpu.CompilerParams(vmem_limit_bytes=vmem_mib << 20, **kw)


def cost(gflops, mbytes):
    return pl.CostEstimate(flops=gflops * 10**9, bytes_accessed=mbytes * 10**6, transcendentals=0)


def whole(shape):
    zeros = (0,) * len(shape)
    return pl.BlockSpec(shape, lambda *_: zeros)


def route_masks(pos_row, rows):
    return [iota((rows, pos.shape[COL]), ROW) == pos for pos in pair_of(pos_row, ROW)]


def expert_rows(off, expert, blk, body):
    start = off[expert]
    count = off[expert + 1] - start

    def step(i, carry):
        body(pl.multiple_of(start + i * blk, TILE))
        return carry

    lax.fori_loop(0, (count + blk - 1) // blk, step, 0)


class ExpertWeights:
    def __init__(self, refs, mine):
        self.gate_refs, self.up_refs, down = refs[:2], refs[2:4], refs[4:]
        self.half_ff = down[0].shape[2]
        self.cores = [(pl.multiple_of(core * self.half_ff, TILE), ref) for core, ref in zip((mine, 1 - mine), down)]

    def rows_of(self, core):
        return pl.ds(core[0], self.half_ff)

    def wide(self, refs, core):
        return jnp.concatenate([ref[0, 0, self.rows_of(core)] for ref in refs], axis=COL)

    def gate(self, core):
        return self.wide(self.gate_refs, core)

    def up(self, core):
        return self.wide(self.up_refs, core)

    def down(self, core):
        return get(core[1]).reshape(self.half_ff, -1)


def moe_fwd_kernel(off, fs, x_ref, gain_ref, wr_ref, prow_ref, pcol_ref, ecol_ref, *refs, rows, blk):
    w_refs, (out_ref, xs_out, y0_out, y1_out, xs_s, down_s) = refs[:6], refs[6:]
    expert = pl.program_id(0)
    toks = x_ref.shape[ROW]
    weights = ExpertWeights(w_refs, fs[0])

    @pl.when(expert == 0)
    def _():
        normed = rms_norm(get(x_ref), get(gain_ref))
        hit0, hit1 = route_masks(get(prow_ref), rows)
        xs = dot(hot(hit0 | hit1), normed).astype(BF16)
        put(xs_out, xs)
        xs_s[:rows] = own_first(xs, fs[0])
        xs_s[rows:] = jnp.zeros((blk, xs.shape[COL]), BF16)
        fill(down_s, 0)

    def body(at):
        xs = xs_s[pl.ds(at, blk)]
        out = down_s.at[pl.ds(at, blk)]

        def hidden(core):
            gate = dot_nt(weights.gate(core), xs)
            return (gate * jax.nn.sigmoid(gate) * dot_nt(weights.up(core), xs)).astype(BF16)

        downs = []
        staggered(weights.cores, hidden, lambda core, made: downs.append(dot_tn(made, weights.down(core))))
        put(out, functools.reduce(jnp.add, downs))

    expert_rows(off, expert, blk, body)

    @pl.when(expert == pl.num_programs(0) - 1)
    def _():
        x = get(x_ref)
        logits = dot_nt(rms_norm(x, get(gain_ref)), get(wr_ref))
        gates = pair_gates(logits, get(ecol_ref), COL)
        col_id = iota((toks, rows), COL)
        hi, mid, lo = split3(down_s[:rows])
        for slot, gate, y_out in zip(pair_of(get(pcol_ref), COL), gates, (y0_out, y1_out)):
            pick = hot(col_id == slot)
            y = dot(pick, hi) + dot(pick, mid) + dot(pick, lo)
            put(y_out, y)
            x = x + y * gate
        put(out_ref, x)


def pair_gates(logits, experts, axis):
    ids = iota(logits.shape, axis)
    r0, r1 = [axis_sum(keep(ids == chosen, logits), axis) for chosen in pair_of(experts, axis)]
    top = jnp.maximum(r0, r1)
    e0 = jnp.exp(r0 - top)
    e1 = jnp.exp(r1 - top)
    return e0 / (e0 + e1), e1 / (e0 + e1)


def moe_bwd_kernel(off, fs, dx_ref, x_ref, gain_ref, wr_ref, prow_ref, pcol_ref, erow_ref, ecol_ref, y0_ref, y1_ref, xs_ref, *refs, rows, blk):
    w_refs, (dx_out, dys_out, dwr_out, dg_out, xs_s, dys_s, dxs_s) = refs[:6], refs[6:]
    expert = pl.program_id(0)
    toks, width = x_ref.shape
    mine = fs[0]
    weights = ExpertWeights(w_refs, mine)

    @pl.when(expert == 0)
    def _():
        normed = rms_norm(get(x_ref), get(gain_ref))
        gate0, gate1 = pair_gates(dot_nt(get(wr_ref), normed), get(erow_ref), ROW)
        hit0, hit1 = route_masks(get(prow_ref), rows)
        gate_rows = axis_sum(keep(hit0, gate0) + keep(hit1, gate1), COL)
        dys = select_rows(hot(hit0 | hit1), get(dx_ref)) * gate_rows
        put(dys_out, dys)
        tail = jnp.zeros((blk, width), BF16)
        dys_s[:rows] = dys.astype(BF16)
        dys_s[rows:] = tail
        xs_s[:rows] = own_first(get(xs_ref), mine)
        xs_s[rows:] = tail
        fill(dxs_s, 0)

    def body(at):
        xs = xs_s[pl.ds(at, blk)]
        dys = dys_s[pl.ds(at, blk)]

        def gradients(core):
            gate = dot_nt(weights.gate(core), xs)
            up = dot_nt(weights.up(core), xs)
            return glu_bwd(gate, up, dot_nt(weights.down(core), dys))

        parts = []

        def back(core, made):
            d_gate, d_up, _ = made
            parts.extend([dot_tn(d_gate, weights.gate(core)), dot_tn(d_up, weights.up(core))])

        staggered(weights.cores, gradients, back)
        dxs_s[pl.ds(at, blk)] = functools.reduce(jnp.add, parts)

    expert_rows(off, expert, blk, body)

    @pl.when(expert == pl.num_programs(0) - 1)
    def _():
        x = get(x_ref)
        dx = get(dx_ref)
        gain = get(gain_ref)
        normed = rms_norm(x, gain)
        logits = dot_nt(normed, get(wr_ref))
        experts = get(ecol_ref)
        gate0, gate1 = pair_gates(logits, experts, COL)
        d_gate0 = axis_sum(dx * get(y0_ref), COL)
        d_gate1 = axis_sum(dx * get(y1_ref), COL)
        mean = gate0 * d_gate0 + gate1 * d_gate1
        first, second = pair_of(experts, COL)
        ids = iota(logits.shape, COL)
        d_logits = (keep(ids == first, gate0 * (d_gate0 - mean)) + keep(ids == second, gate1 * (d_gate1 - mean))).astype(BF16)
        put(dwr_out, dot_tn(d_logits, normed))
        col_id = iota((toks, rows), COL)
        slot0, slot1 = pair_of(get(pcol_ref), COL)
        d_normed = own_first(select_rows(hot((col_id == slot0) | (col_id == slot1)), dxs_s[:rows]), mine) + dot(d_logits, get(wr_ref))
        d_x, d_gain = rms_norm_bwd(x, gain, d_normed.astype(BF16).astype(F32))
        put(dx_out, dx + d_x)
        put(dg_out, d_gain)


def glu_bwd(gate, up, d_hidden):
    sig = jax.nn.sigmoid(gate)
    act = gate * sig
    d_gate = (d_hidden * up * (sig + act * (1.0 - sig))).astype(BF16)
    d_up = (d_hidden * act).astype(BF16)
    return d_gate, d_up, (act * up).astype(BF16)


def expert_specs(layer, weights):
    return [pl.BlockSpec((1, 1, *w.shape[2:]), lambda e, *_: (layer, e, 0, 0)) for w in weights]


def moe_fwd(layer, off, fs, x, gain, w_r, pos_row, pos_col, exp_col, weights, rows):
    toks, width = x.shape
    blk = LANES
    tok_out = jax.ShapeDtypeStruct((toks, width), F32)
    out_shapes = (tok_out, jax.ShapeDtypeStruct((rows, width), BF16), tok_out, tok_out)
    small = [x, gain, w_r, pos_row, pos_col, exp_col]
    return pl.pallas_call(
        functools.partial(moe_fwd_kernel, rows=rows, blk=blk),
        out_shape=out_shapes,
        grid_spec=pltpu.PrefetchScalarGridSpec(
            num_scalar_prefetch=2,
            grid=(w_r.shape[ROW],),
            in_specs=[whole(a.shape) for a in small] + expert_specs(layer, weights),
            out_specs=tuple(whole(s.shape) for s in out_shapes),
            scratch_shapes=[pltpu.VMEM((rows + blk, width), BF16), pltpu.VMEM((rows + blk, width), F32)],
        ),
        compiler_params=params(48),
        cost_estimate=cost(30, 45),
        name="moe_fwd",
    )(off, fs, *small, *weights)


def moe_bwd(layer, off, fs, dx, x, gain, w_r, pos_row, pos_col, exp_row, exp_col, y0, y1, xs, weights, rows):
    toks, width = x.shape
    blk = LANES
    small = [dx, x, gain, w_r, pos_row, pos_col, exp_row, exp_col, y0, y1, xs]
    out_shapes = tuple(jax.ShapeDtypeStruct((count, width), F32) for count in (toks, rows, w_r.shape[ROW], 1))
    buffer = pltpu.VMEM((rows + blk, width), BF16)
    return pl.pallas_call(
        functools.partial(moe_bwd_kernel, rows=rows, blk=blk),
        out_shape=out_shapes,
        grid_spec=pltpu.PrefetchScalarGridSpec(
            num_scalar_prefetch=2,
            grid=(w_r.shape[ROW],),
            in_specs=[whole(a.shape) for a in small] + expert_specs(layer, weights),
            out_specs=tuple(whole(s.shape) for s in out_shapes),
            scratch_shapes=[buffer, buffer, pltpu.VMEM((rows + blk, width), F32)],
        ),
        compiler_params=params(60),
        cost_estimate=cost(50, 50),
        name="moe_bwd",
    )(off, fs, *small, *weights)


def expert_dw_kernel(off, fs, lr_ref, xs_hbm, dys_hbm, *refs, blk, alias):
    w_refs, masters, refs = refs[:6], refs[6:9], refs[12 if alias else 9 :]
    outs, (xbuf, dbuf, sems), accs = refs[:3], refs[3:6], refs[6:]
    acc_g, acc_u, acc_d = accs
    expert = pl.program_id(0)
    seqs = xs_hbm.shape[0]
    half = acc_g.shape[COL]
    mine = fs[0]
    weights = ExpertWeights(w_refs, mine)

    def copies(e, slot, act):
        at = 0
        for s in range(seqs):
            start = pl.multiple_of(off[s, e], TILE)
            count = pl.multiple_of(off[s, e + 1] - off[s, e], TILE)
            target = pl.ds(pl.multiple_of(at, TILE), count)

            @pl.when(count > 0)
            def _():
                for k, (hbm, buf) in enumerate(((xs_hbm, xbuf), (dys_hbm, dbuf))):
                    act(pltpu.make_async_copy(hbm.at[s, pl.ds(start, count)], buf.at[slot, target], sems.at[slot, k]))

            at = at + count
        return at

    slot = lax.rem(expert, 2)

    @pl.when(expert == 0)
    def _():
        copies(0, 0, lambda copy: copy.start())

    @pl.when(expert + 1 < pl.num_programs(0))
    def _():
        copies(expert + 1, 1 - slot, lambda copy: copy.start())

    total = pl.multiple_of(copies(expert, slot, lambda copy: copy.wait()), TILE)
    for buf in (xbuf, dbuf):
        buf[slot, pl.ds(total, blk)] = jnp.zeros((blk, buf.shape[2]), buf.dtype)
    for acc in accs:
        fill(acc, 0)

    def body(i, carry):
        rows = pl.ds(pl.multiple_of(i * blk, blk), blk)
        xs = own_first(xbuf[slot, rows], mine)
        dys = dbuf[slot, rows].astype(BF16)
        own, xs_t, dys_t = xs[:, :half], xs.T, dys.T

        def gradients(core):
            return glu_bwd(dot(weights.gate(core), xs_t), dot(weights.up(core), xs_t), dot(weights.down(core), dys_t))

        def add(core, made):
            d_gate, d_up, hidden = made
            part = weights.rows_of(core)
            acc_g[part] += dot(d_gate, own)
            acc_u[part] += dot(d_up, own)
            if core is weights.cores[0]:
                put(acc_d, get(acc_d) + dot(hidden, dys))

        staggered(weights.cores, gradients, add)
        return carry

    lax.fori_loop(0, (total + blk - 1) // blk, body, 0)
    for out, master, acc in zip(outs, masters, accs):
        put(out, get(master) - get(lr_ref) * get(acc).reshape(out.shape))


def expert_dw(layer, off, fs, lr, xs, dys, weights, masters, prev):
    seqs, _, width = xs.shape
    experts = masters[0].shape[1]
    blk = 2 * LANES
    most = seqs * width + blk
    any_spec = pl.BlockSpec(memory_space=pl.ANY)
    specs = expert_specs(layer, masters)
    alias = prev is not None
    in_specs = [whole(lr.shape), any_spec, any_spec] + expert_specs(layer, weights) + specs
    in_specs += [any_spec] * 3 if alias else []
    first_prev = len(in_specs) - 1
    return pl.pallas_call(
        functools.partial(expert_dw_kernel, blk=blk, alias=alias),
        out_shape=tuple(jax.ShapeDtypeStruct(m.shape, F32) for m in masters),
        grid_spec=pltpu.PrefetchScalarGridSpec(
            num_scalar_prefetch=2,
            grid=(experts,),
            in_specs=in_specs,
            out_specs=tuple(specs),
            scratch_shapes=[
                pltpu.VMEM((2, most, width), BF16),
                pltpu.VMEM((2, most, width), F32),
                pltpu.SemaphoreType.DMA((2, 2)),
            ]
            + [pltpu.VMEM(m.shape[2:], F32) for m in masters],
        ),
        input_output_aliases={first_prev + k: k for k in range(3)} if alias else {},
        compiler_params=params(62),
        cost_estimate=cost(60, 150),
        name="expert_dw",
    )(off, fs, lr, xs, dys, *weights, *masters, *(prev or ()))


def head_kernel(fs, x_ref, gain_ref, lab_ref, wa_ref, wb_ref, fin_out, lse_out, dx_out, dg_out, loss_out, fin_s, top_s, sum_s, pick_s, acc_s, *, tokens_all):
    sweep = pl.program_id(0)
    step = pl.program_id(1)
    last = pl.num_programs(1) - 1
    tile = wa_ref.shape[ROW]
    mine = fs[0]
    parts = pieces(tile, HEAD_PIECE)

    @pl.when((sweep == 0) & (step == 0))
    def _():
        fin = rms_norm(get(x_ref), get(gain_ref))
        put(fin_out, fin)
        put(fin_s, own_first(fin, mine).T)
        fill(top_s, NEG)
        fill(sum_s, 0)
        fill(pick_s, 0)
        fill(acc_s, 0)

    def logits_of(part):
        return dot(both_cores((wa_ref, wb_ref), *part), get(fin_s)) * LOG2E

    def take_sums(part, logits):
        grouped = sublane_groups(logits)
        old = get(top_s)
        new = jnp.maximum(old, jnp.max(grouped, axis=ROW))
        put(sum_s, get(sum_s) * jnp.exp2(old - new) + jnp.sum(jnp.exp2(grouped - new), axis=ROW))
        put(top_s, new)

    @pl.when(sweep == 0)
    def _():
        staggered(parts, logits_of, take_sums)

    @pl.when((sweep == 0) & (step == last))
    def _():
        top = jnp.max(get(top_s), axis=ROW, keepdims=True)
        total = axis_sum(get(sum_s) * jnp.exp2(get(top_s) - top), ROW)
        put(lse_out, jnp.broadcast_to(top + jnp.log2(total), lse_out.shape))

    def gradient(part):
        logits = logits_of(part)
        prob = jnp.exp2(logits - (lse_out[:1] + jnp.log2(jnp.float32(tokens_all))))
        hit = iota(logits.shape, ROW) == get(lab_ref) - (step * tile + part[0])
        put(pick_s, get(pick_s) + jnp.sum(sublane_groups(keep(hit, logits)), axis=ROW))
        return (prob - jnp.where(hit, 1.0 / tokens_all, 0.0)).astype(BF16)

    def add_gradient(part, grad):
        put(acc_s, get(acc_s) + dot_tn(grad, both_cores((wa_ref, wb_ref), *part)))

    @pl.when(sweep == 1)
    def _():
        staggered(parts, gradient, add_gradient)

    @pl.when((sweep == 1) & (step == last))
    def _():
        per_tok = (lse_out[:1] - axis_sum(get(pick_s), ROW)) * (LN2 / tokens_all)
        put(loss_out, jnp.broadcast_to(axis_sum(per_tok, COL), loss_out.shape))
        d_fin = own_first(get(acc_s), mine).astype(BF16).astype(F32)
        d_x, d_gain = rms_norm_bwd(get(x_ref), get(gain_ref), d_fin)
        put(dx_out, d_x)
        put(dg_out, d_gain)


def head(fs, x, gain, labels, w_own, w_other, tokens_all):
    toks, width = x.shape
    vocab, half = w_own.shape
    tile = vocab // HEAD_STEPS
    out_shapes = (
        jax.ShapeDtypeStruct((toks, width), BF16),
        jax.ShapeDtypeStruct((LSE_ROWS, toks), F32),
        jax.ShapeDtypeStruct((toks, width), F32),
        jax.ShapeDtypeStruct((1, width), F32),
        jax.ShapeDtypeStruct((1, width), F32),
    )
    small = [x, gain, labels]
    w_spec = pl.BlockSpec((tile, half), lambda p, i, *_: (i, 0))
    return pl.pallas_call(
        functools.partial(head_kernel, tokens_all=tokens_all),
        out_shape=out_shapes,
        grid_spec=pltpu.PrefetchScalarGridSpec(
            num_scalar_prefetch=1,
            grid=(2, HEAD_STEPS),
            in_specs=[whole(a.shape) for a in small] + [w_spec, w_spec],
            out_specs=tuple(whole(s.shape) for s in out_shapes),
            scratch_shapes=[pltpu.VMEM((width, toks), BF16)] + [pltpu.VMEM((SUBLANES, toks), F32)] * 3 + [pltpu.VMEM((toks, width), F32)],
        ),
        compiler_params=params(56),
        cost_estimate=cost(55, 70),
        name="head_own",
    )(fs, *small, w_own, w_other)


def head_dw_kernel(fs, lr_ref, fin_ref, lse_ref, lab_ref, wa_ref, wb_ref, m_ref, new_out, oth_out, fin_s, fin_t, acc_s, *, tokens_all):
    tile, half = wa_ref.shape
    seqs = fin_s.shape[0]
    mine = fs[0]
    base = (mine * pl.num_programs(0) + pl.program_id(0)) * tile
    parts = pieces(tile, DW_PIECE)
    fill(acc_s, 0)
    fill(oth_out, 0)

    @pl.when(pl.program_id(0) == 0)
    def _():
        for s in range(seqs):
            fin = own_first(fin_ref[s], mine)
            fin_s[s] = fin
            fin_t[s] = fin.T

    def body(s, carry):
        lse = lse_ref[s, :1] + jnp.log2(jnp.float32(tokens_all))
        lab = lab_ref[s] - base

        def gradient(part):
            logits = dot(both_cores((wa_ref, wb_ref), *part), fin_t[s]) * LOG2E
            hit = iota(logits.shape, ROW) == lab - part[0]
            return (jnp.exp2(logits - lse) - jnp.where(hit, 1.0 / tokens_all, 0.0)).astype(BF16)

        def add_gradient(part, grad):
            rows = slice(*part)
            acc_s[rows] += dot(grad, fin_s[s, :, :half])
            oth_out[rows] += dot(grad, fin_s[s, :, half:])

        staggered(parts, gradient, add_gradient)
        return carry

    lax.fori_loop(0, seqs, body, 0)
    put(new_out, get(m_ref) - get(lr_ref) * get(acc_s))


def head_dw(fs, lr, fin, lse, labels, w_own, w_other, master, tokens_all):
    seqs, toks, width = fin.shape
    vocab, half = master.shape
    steps = HEAD_STEPS // 2
    tile = vocab // HEAD_STEPS
    spec = pl.BlockSpec((tile, half), lambda i, f: (f[0] * steps + i, 0))
    small = [lr, fin, lse, labels]
    return pl.pallas_call(
        functools.partial(head_dw_kernel, tokens_all=tokens_all),
        out_shape=(jax.ShapeDtypeStruct((vocab, half), F32), jax.ShapeDtypeStruct((steps * tile, half), F32)),
        grid_spec=pltpu.PrefetchScalarGridSpec(
            num_scalar_prefetch=1,
            grid=(steps,),
            in_specs=[whole(a.shape) for a in small] + [spec] * 3,
            out_specs=(spec, pl.BlockSpec((tile, half), lambda i, *_: (i, 0))),
            scratch_shapes=[
                pltpu.VMEM((seqs, toks, width), BF16),
                pltpu.VMEM((seqs, width, toks), BF16),
                pltpu.VMEM((tile, half), F32),
            ],
        ),
        compiler_params=params(60),
        cost_estimate=cost(140, 70),
        name="head_dw",
    )(fs, *small, w_own, w_other, master)


def head_upd_kernel(fs, lr_ref, grad_ref, m_ref, prev_ref, new_out):
    put(new_out, get(m_ref) - get(lr_ref) * get(grad_ref))


def head_upd(fs, lr, grad, master, prev):
    vocab, half = master.shape
    steps = HEAD_STEPS // 2
    tile = vocab // HEAD_STEPS
    spec = pl.BlockSpec((tile, half), lambda i, f: ((1 - f[0]) * steps + i, 0))
    return pl.pallas_call(
        head_upd_kernel,
        out_shape=jax.ShapeDtypeStruct((vocab, half), F32),
        grid_spec=pltpu.PrefetchScalarGridSpec(
            num_scalar_prefetch=1,
            grid=(steps,),
            in_specs=[whole(lr.shape), pl.BlockSpec((tile, half), lambda i, *_: (i, 0)), spec, pl.BlockSpec(memory_space=pl.ANY)],
            out_specs=spec,
        ),
        input_output_aliases={4: 0},
        compiler_params=params(48),
        cost_estimate=cost(15, 50),
        name="head_upd",
    )(fs, lr, grad, master, prev)


def embed_upd_kernel(bounds, keys, perm, lr_ref, rows_ref, m_ref, new_out, wide_s):
    step = pl.program_id(0)
    rows = m_ref.shape[0]

    @pl.when(step == 0)
    def _():
        put(wide_s, get(rows_ref).astype(F32) * get(lr_ref))

    put(new_out, get(m_ref))

    def body(j, carry):
        at = new_out.at[pl.ds(keys[j] - step * rows, 1)]
        put(at, get(at) - get(wide_s.at[pl.ds(perm[j], 1)]))
        return carry

    lax.fori_loop(bounds[step], bounds[step + 1], body, 0)


def embed_upd(bounds, keys, perm, lr, grads, master, rows):
    vocab, width = master.shape
    return pl.pallas_call(
        embed_upd_kernel,
        out_shape=jax.ShapeDtypeStruct((vocab, width), F32),
        grid_spec=pltpu.PrefetchScalarGridSpec(
            num_scalar_prefetch=3,
            grid=(vocab // rows,),
            in_specs=[
                whole(lr.shape),
                whole(grads.shape),
                pl.BlockSpec((rows, width), lambda i, *_: (i, 0)),
            ],
            out_specs=pl.BlockSpec((rows, width), lambda i, *_: (i, 0)),
            scratch_shapes=[pltpu.VMEM(grads.shape, F32)],
        ),
        compiler_params=params(48),
        cost_estimate=cost(25, 66),
        name="embed_upd",
    )(bounds, keys, perm, lr, grads, master)


def rope_tables(positions):
    inv_freq = ROPE_THETA ** (-jnp.arange(0, HEAD_DIM, 2, dtype=F32) / HEAD_DIM)
    angle = positions.astype(F32)[:, None] * inv_freq
    cos, sin = jnp.cos(angle), jnp.sin(angle)
    return jnp.concatenate([cos, cos], axis=COL), jnp.concatenate([-sin, sin], axis=COL)


def half_turn(x):
    return pltpu.roll(x, HEAD_DIM // 2, COL)


def rope(x, cos, sin):
    return x * cos + half_turn(x) * sin


def rope_bwd(dx, cos, sin):
    return dx * cos + half_turn(dx * sin)


def qkv_heads(x, gain, weights, cos, sin, q_width):
    normed = rms_norm(x, gain)
    all_heads = jnp.split(dot(normed, weights), weights.shape[COL] // HEAD_DIM, axis=COL)
    count = q_width // HEAD_DIM
    queries = [rope(q, cos, sin).astype(BF16) for q in all_heads[:count]]
    key, value = all_heads[count:]
    return normed, queries, rope(key, cos, sin).astype(BF16), value.astype(BF16)


def attn_probs(query, key):
    scores = dot_nt(query, key) * HEAD_DIM ** -0.5
    scores = jnp.where(iota(scores.shape, ROW) >= iota(scores.shape, COL), scores, NEG)
    raised = jnp.exp(scores - jnp.max(scores, axis=COL, keepdims=True))
    return raised / axis_sum(raised, COL)


def attn_fwd_kernel(x_ref, gain_ref, cos_ref, sin_ref, w_ref, out_ref, *, q_width, in_width):
    x = get(x_ref)
    weights = get(w_ref).reshape(x.shape[COL], -1)
    _, queries, key, value = qkv_heads(x, get(gain_ref), weights[:, :in_width], get(cos_ref), get(sin_ref), q_width)
    mixed = [dot(attn_probs(query, key).astype(BF16), value).astype(BF16) for query in queries]
    put(out_ref, x + dot(jnp.concatenate(mixed, axis=COL), weights[:, in_width:]))


def attn_bwd_kernel(dx_ref, x_ref, gain_ref, cos_ref, sin_ref, dwr_ref, dgm_ref, dgf_ref, loss_ref, w_ref, dx_out, dw_out, *, q_width, in_width):
    x = get(x_ref)
    d_out = get(dx_ref)
    gain, cos, sin = get(gain_ref), get(cos_ref), get(sin_ref)
    weights = get(w_ref).reshape(x.shape[COL], -1)
    half = x.shape[COL] // 2
    normed, queries, key, value = qkv_heads(x, gain, weights[:, :in_width], cos, sin, q_width)
    d_proj = d_out.astype(BF16)
    d_mixed = jnp.split(dot_nt(d_proj, weights[:, in_width:]).astype(BF16), len(queries), axis=COL)
    mixed, d_heads = [], []
    d_key = d_value = None
    for query, d_mix in zip(queries, d_mixed):
        probs = attn_probs(query, key)
        rounded = probs.astype(BF16)
        mixed.append(dot(rounded, value).astype(BF16))
        d_probs = dot_nt(d_mix, value)
        d_scores = (probs * (d_probs - axis_sum(d_probs * probs, COL)) * HEAD_DIM ** -0.5).astype(BF16)
        d_heads.append(rope_bwd(dot(d_scores, key), cos, sin).astype(BF16))
        more_key, more_value = dot_tn(d_scores, query), dot_tn(rounded, d_mix)
        d_key = more_key if d_key is None else d_key + more_key
        d_value = more_value if d_value is None else d_value + more_value
    d_heads += [rope_bwd(d_key, cos, sin).astype(BF16), d_value.astype(BF16)]
    d_in = jnp.concatenate(d_heads, axis=COL)
    d_weights = jnp.concatenate([dot_tn(normed, d_in), dot_tn(jnp.concatenate(mixed, axis=COL), d_proj)], axis=COL)
    d_x, d_gain = rms_norm_bwd(x, gain, dot_nt(d_in, weights[:, :in_width]).astype(BF16).astype(F32))
    put(dx_out, d_out + d_x)
    for core, d_half in enumerate(pair_of(d_weights, ROW)):
        dw_out[core, :half] = d_half
    small = jnp.concatenate([get(dwr_ref), d_gain, get(dgm_ref), get(dgf_ref), get(loss_ref)], axis=ROW)
    per_row = d_weights.shape[COL] // half
    for i in range(small.shape[ROW]):
        row, at = half + i // per_row, i % per_row * half
        for core, part in enumerate(pair_of(small[i : i + 1], COL)):
            dw_out[core, row : row + 1, at : at + half] = part


def attn_specs(arrays, w_all, layer):
    spec = pl.BlockSpec((2, 1, *w_all.shape[2:]), lambda i: (0, layer, 0, 0))
    return [whole(a.shape) for a in arrays] + [spec]


def attn_fwd(layer, x, gain, cos, sin, w_all, q_width, in_width):
    small = [x, gain, cos, sin]
    return pl.pallas_call(
        functools.partial(attn_fwd_kernel, q_width=q_width, in_width=in_width),
        out_shape=jax.ShapeDtypeStruct(x.shape, F32),
        grid=(1,),
        in_specs=attn_specs(small, w_all, layer),
        out_specs=whole(x.shape),
        compiler_params=params(48),
        cost_estimate=cost(8, 5),
        name="attn_fwd",
    )(*small, w_all)


def attn_bwd(layer, dx, x, gain, cos, sin, d_router, d_mlp, d_final, loss, w_all, q_width, in_width):
    small = [dx, x, gain, cos, sin, d_router, d_mlp, d_final, loss]
    half, wide = w_all.shape[2:]
    tail = -(-(d_router.shape[ROW] + 4) // (wide // half) // SUBLANES) * SUBLANES
    grads = jax.ShapeDtypeStruct((2, half + tail, wide), F32)
    return pl.pallas_call(
        functools.partial(attn_bwd_kernel, q_width=q_width, in_width=in_width),
        out_shape=(jax.ShapeDtypeStruct(x.shape, F32), grads),
        grid=(1,),
        in_specs=attn_specs(small, w_all, layer),
        out_specs=(whole(x.shape), whole(grads.shape)),
        compiler_params=params(60),
        cost_estimate=cost(15, 10),
        name="attn_bwd",
    )(*small, w_all)


def routing(experts_of, experts):
    toks = experts_of.shape[0]
    hot = (experts_of[:, :, None] == jnp.arange(experts, dtype=I32)).astype(F32)
    both = hot[:, 0] + hot[:, 1]
    before = iota((toks, toks), 0) > iota((toks, toks), 1)
    ahead = dot(before.astype(BF16), both.astype(BF16))
    counts = jnp.sum(both, axis=0).astype(I32)
    padded = (counts + TILE - 1) // TILE * TILE
    upto = iota((experts + 1, experts), 0) > iota((experts + 1, experts), 1)
    starts = jnp.sum(jnp.where(upto, padded[None, :], 0), axis=1)
    place = starts[:experts].astype(F32) + ahead
    return jnp.sum(hot * place[:, None, :], axis=2).astype(I32), starts


def solution(mesh):
    device_count = mesh.shape['rep'] * mesh.shape['fsdp']
    both = ('rep', 'fsdp')
    batch_spec = P(both)
    layer_spec = P(None, 'fsdp')
    expert_spec = P(None, None, 'fsdp')
    param_specs = (P('fsdp'), layer_spec, layer_spec, layer_spec, layer_spec, layer_spec, layer_spec, layer_spec, expert_spec, expert_spec, expert_spec, P('fsdp'), P('fsdp'))
    in_specs = (batch_spec, batch_spec, batch_spec, P(None, both), P()) + param_specs
    out_specs = param_specs + (P(),)

    def step(tok_ids, tok_labels, tok_pos, expert_idx, learn_rate, embedding, w_query, w_key, w_value, w_attn_out, g_attn, g_mlp, w_router, w_gate, w_up, w_down, g_final, w_head):
        layers, half, q_width = w_query.shape
        kv_width = w_key.shape[2]
        width = 2 * half
        toks = tok_ids.shape[1]
        experts = w_router.shape[2]
        tokens_all = toks * device_count
        vocab_share = embedding.shape[0]
        rows = 2 * toks + experts * TILE
        me = lax.axis_index('fsdp')
        pair = lax.axis_index('rep')
        fs = jnp.stack([me, pair]).astype(I32)
        lr = learn_rate.reshape(1, 1)
        swap = [(0, 1), (1, 0)]

        m_gate = jnp.swapaxes(w_gate, 2, 3)
        m_up = jnp.swapaxes(w_up, 2, 3)
        m_head = w_head.T

        experts_of = expert_idx[:, 0]
        placed = [routing(experts_of[l], experts) for l in range(layers)]
        starts = jnp.stack([s for _, s in placed])
        ints = jnp.concatenate([tok_ids[0], tok_labels[0], starts.reshape(-1)]).astype(F32)
        misc = jnp.concatenate([jnp.swapaxes(w_router, 1, 2).reshape(layers * experts, half), g_attn, g_mlp, g_final[None]])
        misc = misc.astype(BF16).astype(F32).reshape(-1)
        packed = jnp.concatenate([misc, ints])
        n_misc = misc.shape[0]
        packed = jnp.pad(packed, (0, KNOWN - packed.shape[0])).reshape(-1, LANES)
        known = lax.all_gather(packed, both).reshape(device_count, -1)
        two = lax.dynamic_slice_in_dim(known, pair * 2, 2, 0)[:, :n_misc].reshape(2, -1, half)
        misc_all = jnp.concatenate([two[0], two[1]], axis=1)
        w_r = [misc_all[l * experts : (l + 1) * experts].astype(BF16) for l in range(layers)]
        base = layers * experts
        gain_attn = [misc_all[base + l][None] for l in range(layers)]
        gain_mlp = [misc_all[base + layers + l][None] for l in range(layers)]
        gain_final = misc_all[base + 2 * layers][None]
        known_ints = known[:, n_misc : n_misc + ints.shape[0]].astype(I32)
        ids_all = known_ints[:, :toks]
        labels_all = known_ints[:, toks : 2 * toks]
        starts_all = known_ints[:, 2 * toks :].reshape(device_count, layers, experts + 1)

        attn_pack = jnp.concatenate([w_query, w_key, w_value, w_attn_out], axis=2).astype(BF16)
        attn_all = lax.all_gather(attn_pack, 'fsdp')

        def with_partner(x):
            rounded = x.astype(BF16)
            return rounded, lax.ppermute(rounded, 'fsdp', swap)

        expert_w = with_partner(m_gate) + with_partner(m_up) + with_partner(w_down)
        head_w = with_partner(m_head)

        partner_ids = lax.dynamic_index_in_dim(ids_all, pair * 2 + 1 - me, 0, keepdims=False)
        wanted = jnp.concatenate([tok_ids[0], partner_ids]) - me * vocab_share
        taken = jnp.take(embedding, jnp.clip(wanted, 0, vocab_share - 1), axis=0).astype(BF16)
        sent = lax.ppermute(taken[toks:], 'fsdp', swap)
        is_mine = (wanted[:toks] >= 0) & (wanted[:toks] < vocab_share)
        x = jnp.where(is_mine[:, None], taken[:toks], sent).astype(F32)

        tables = rope_tables(tok_pos[0])
        widths = (q_width, q_width + 2 * kv_width)

        xs_all, kept = [], []
        for l in range(layers):
            mid = attn_fwd(l, x, gain_attn[l], *tables, attn_all, *widths)
            pos, start = placed[l]
            out, xs, y0, y1 = moe_fwd(l, start, fs, mid, gain_mlp[l], w_r[l], pos.T, pos, experts_of[l], expert_w, rows)
            kept.append((x, mid, xs, y0, y1))
            xs_all.append(lax.all_gather(xs, both))
            x = out

        fin, lse, dx, d_final, loss = head(fs, x, gain_final, tok_labels, *head_w, tokens_all)
        fin_all = lax.all_gather(fin, both)
        lse_all = lax.all_gather(lse, both)

        dys_all = [None] * layers
        reduced = [None] * layers
        for l in reversed(range(layers)):
            x, mid, xs, y0, y1 = kept[l]
            pos, start = placed[l]
            dx, dys, d_router, d_mlp = moe_bwd(l, start, fs, dx, mid, gain_mlp[l], w_r[l], pos.T, pos, experts_of[l].T, experts_of[l], y0, y1, xs, expert_w, rows)
            dys_all[l] = lax.all_gather(dys, both)
            dx, grads = attn_bwd(l, dx, x, gain_attn[l], *tables, d_router, d_mlp, d_final, loss, attn_all, *widths)
            reduced[l] = lax.psum(lax.psum_scatter(grads, 'fsdp', scatter_dimension=0, tiled=False), 'rep')

        d_rows = lax.all_gather(dx.astype(BF16), both).reshape(tokens_all, width)

        fin_all, _ = lax.optimization_barrier((fin_all, dx))
        new_head, other_grad = head_dw(fs, lr, fin_all, lse_all, labels_all[:, None], *head_w, m_head, tokens_all)
        other_grad = lax.ppermute(other_grad, 'fsdp', swap)
        new_experts = None
        for l in reversed(range(layers)):
            new_experts = expert_dw(l, starts_all[:, l], fs, lr, xs_all[l], dys_all[l], expert_w, (m_gate, m_up, w_down), new_experts)

        new_head = head_upd(fs, lr, other_grad, m_head, new_head)

        block = 1336
        local_id = ids_all.reshape(-1) - me * vocab_share
        key = jnp.where((local_id >= 0) & (local_id < vocab_share), local_id, vocab_share)
        keys, perm = lax.sort((key, lax.iota(I32, tokens_all)), num_keys=1)
        edges = jnp.arange(vocab_share // block + 1, dtype=I32) * block
        bounds = jnp.sum(key[None, :] < edges[:, None], axis=1).astype(I32)
        new_embedding = embed_upd(bounds, keys, perm, lr, d_rows, embedding, block)

        def update(master, pick):
            return master - learn_rate * jnp.stack([pick(reduced[l]) for l in range(layers)])

        def tail_of(r, first, count):
            return r[half:].reshape(-1)[first * half : (first + count) * half].reshape(count, half)

        v_at = q_width + kv_width
        new_query = update(w_query, lambda r: r[:half, :q_width])
        new_key = update(w_key, lambda r: r[:half, q_width:v_at])
        new_value = update(w_value, lambda r: r[:half, v_at : v_at + kv_width])
        new_attn_out = update(w_attn_out, lambda r: r[:half, v_at + kv_width :])
        new_router = update(w_router, lambda r: tail_of(r, 0, experts).T)
        new_g_attn = update(g_attn, lambda r: tail_of(r, experts, 1)[0])
        new_g_mlp = update(g_mlp, lambda r: tail_of(r, experts + 1, 1)[0])
        new_final = g_final - learn_rate * tail_of(reduced[0], experts + 2, 1)[0]
        both_loss = tail_of(reduced[0], experts + 3, 1)[0, 0]
        new_gate, new_up, new_down = new_experts
        return (new_embedding, new_query, new_key, new_value, new_attn_out, new_g_attn, new_g_mlp, new_router,
                jnp.swapaxes(new_gate, 2, 3), jnp.swapaxes(new_up, 2, 3), new_down, new_final, new_head.T, both_loss)

    return jax.shard_map(step, mesh=mesh, in_specs=in_specs, out_specs=out_specs, check_vma=False)
```

```python
import functools
import jax
import jax.numpy as jnp
from jax import lax
from jax.experimental import pallas as pl
from jax.experimental.pallas import tpu as pltpu
from jax.sharding import PartitionSpec as P

HEAD_DIM = 128
ROPE_THETA = 1000000.0
NORM_EPS = 1e-5
LOG2E = 1.4426950408889634
LN2 = 0.6931471805599453
F32 = jnp.float32
BF16 = jnp.bfloat16
I32 = jnp.int32
TILE = 16
HEAD_STEPS = 12
HEAD_PIECE = 256
DW_PIECE = 384
LSE_ROWS = 72
KNOWN = 40960
SUBLANES = 8
NEG = -1e30
ROW, COL = 0, 1
LANES = 128


def contract(a, b, ca, cb):
    return lax.dot_general(a, b, (((ca,), (cb,)), ((), ())), preferred_element_type=F32)


def dot(a, b):
    return contract(a, b, COL, ROW)


def dot_nt(a, b):
    return contract(a, b, COL, COL)


def dot_tn(a, b):
    return contract(a, b, ROW, ROW)


def get(ref):
    return ref[...]


def put(ref, value):
    ref[...] = value


def fill(ref, value):
    put(ref, jnp.full(ref.shape, value, ref.dtype))


def iota(shape, axis):
    return lax.broadcasted_iota(I32, shape, axis)


def axis_sum(x, axis):
    return jnp.sum(x, axis=axis, keepdims=True)


def keep(mask, x):
    return jnp.where(mask, x, 0.0)


def hot(mask):
    return jnp.where(mask, 1.0, 0.0).astype(BF16)


def pair_of(x, axis):
    return jnp.split(x, 2, axis=axis)


def rms_stats(x):
    return lax.rsqrt(jnp.mean(x * x, axis=-1, keepdims=True) + NORM_EPS)


def rms_norm(x, gain):
    return (x * rms_stats(x) * gain).astype(BF16)


def rms_norm_bwd(x, gain, d_normed):
    inv = rms_stats(x)
    unit = x * inv
    d_gain = axis_sum(d_normed * unit, ROW)
    d_unit = d_normed * gain
    d_x = inv * (d_unit - unit * jnp.mean(d_unit * unit, axis=-1, keepdims=True))
    return d_x, d_gain


def split3(x):
    hi = x.astype(BF16)
    rest = x - hi.astype(F32)
    mid = rest.astype(BF16)
    return hi, mid, (rest - mid.astype(F32)).astype(BF16)


def select_rows(onehot, x):
    hi, mid, lo = split3(x)
    return dot(onehot, hi) + dot(onehot, mid) + dot(onehot, lo)


def pieces(total, size):
    edges = [*range(0, total, size), total]
    return list(zip(edges, edges[1:]))


def staggered(items, first, second):
    held = None
    for item in items:
        made = first(item)
        if held is not None:
            second(*held)
        held = (item, made)
    second(*held)


def own_first(x, mine):
    lower, upper = pair_of(x, COL)
    return jnp.where(mine == 0, x, jnp.concatenate([upper, lower], axis=COL))


def sublane_groups(x):
    return x.reshape(-1, SUBLANES, x.shape[COL])


def both_cores(refs, lo, hi):
    return jnp.concatenate([ref[lo:hi] for ref in refs], axis=COL)


def params(vmem_mib, **kw):
    return pltpu.CompilerParams(vmem_limit_bytes=vmem_mib << 20, **kw)


def cost(gflops, mbytes):
    return pl.CostEstimate(flops=gflops * 10**9, bytes_accessed=mbytes * 10**6, transcendentals=0)


def whole(shape):
    zeros = (0,) * len(shape)
    return pl.BlockSpec(shape, lambda *_: zeros)


def route_masks(pos_row, rows):
    return [iota((rows, pos.shape[COL]), ROW) == pos for pos in pair_of(pos_row, ROW)]


def expert_rows(off, expert, blk, body):
    start = off[expert]
    count = off[expert + 1] - start

    def step(i, carry):
        body(pl.multiple_of(start + i * blk, TILE))
        return carry

    lax.fori_loop(0, (count + blk - 1) // blk, step, 0)


class ExpertWeights:
    def __init__(self, refs, mine):
        self.gate_refs, self.up_refs, down = refs[:2], refs[2:4], refs[4:]
        self.half_ff = down[0].shape[2]
        self.cores = [(pl.multiple_of(core * self.half_ff, TILE), ref) for core, ref in zip((mine, 1 - mine), down)]

    def rows_of(self, core):
        return pl.ds(core[0], self.half_ff)

    def wide(self, refs, core):
        return jnp.concatenate([ref[0, 0, self.rows_of(core)] for ref in refs], axis=COL)

    def gate(self, core):
        return self.wide(self.gate_refs, core)

    def up(self, core):
        return self.wide(self.up_refs, core)

    def down(self, core):
        return get(core[1]).reshape(self.half_ff, -1)


def moe_fwd_kernel(off, fs, x_ref, gain_ref, wr_ref, prow_ref, pcol_ref, ecol_ref, *refs, rows, blk):
    w_refs, (out_ref, xs_out, y0_out, y1_out, xs_s, down_s) = refs[:6], refs[6:]
    expert = pl.program_id(0)
    toks = x_ref.shape[ROW]
    weights = ExpertWeights(w_refs, fs[0])

    @pl.when(expert == 0)
    def _():
        normed = rms_norm(get(x_ref), get(gain_ref))
        hit0, hit1 = route_masks(get(prow_ref), rows)
        xs = dot(hot(hit0 | hit1), normed).astype(BF16)
        put(xs_out, xs)
        xs_s[:rows] = own_first(xs, fs[0])
        xs_s[rows:] = jnp.zeros((blk, xs.shape[COL]), BF16)
        fill(down_s, 0)

    def body(at):
        xs = xs_s[pl.ds(at, blk)]
        out = down_s.at[pl.ds(at, blk)]

        def hidden(core):
            gate = dot_nt(weights.gate(core), xs)
            return (gate * jax.nn.sigmoid(gate) * dot_nt(weights.up(core), xs)).astype(BF16)

        downs = []
        staggered(weights.cores, hidden, lambda core, made: downs.append(dot_tn(made, weights.down(core))))
        put(out, functools.reduce(jnp.add, downs))

    expert_rows(off, expert, blk, body)

    @pl.when(expert == pl.num_programs(0) - 1)
    def _():
        x = get(x_ref)
        logits = dot_nt(rms_norm(x, get(gain_ref)), get(wr_ref))
        gates = pair_gates(logits, get(ecol_ref), COL)
        col_id = iota((toks, rows), COL)
        hi, mid, lo = split3(down_s[:rows])
        for slot, gate, y_out in zip(pair_of(get(pcol_ref), COL), gates, (y0_out, y1_out)):
            pick = hot(col_id == slot)
            y = dot(pick, hi) + dot(pick, mid) + dot(pick, lo)
            put(y_out, y)
            x = x + y * gate
        put(out_ref, x)


def pair_gates(logits, experts, axis):
    ids = iota(logits.shape, axis)
    r0, r1 = [axis_sum(keep(ids == chosen, logits), axis) for chosen in pair_of(experts, axis)]
    top = jnp.maximum(r0, r1)
    e0 = jnp.exp(r0 - top)
    e1 = jnp.exp(r1 - top)
    return e0 / (e0 + e1), e1 / (e0 + e1)


def moe_bwd_kernel(off, fs, dx_ref, x_ref, gain_ref, wr_ref, prow_ref, pcol_ref, erow_ref, ecol_ref, y0_ref, y1_ref, xs_ref, *refs, rows, blk):
    w_refs, (dx_out, dys_out, dwr_out, dg_out, xs_s, dys_s, dxs_s) = refs[:6], refs[6:]
    expert = pl.program_id(0)
    toks, width = x_ref.shape
    mine = fs[0]
    weights = ExpertWeights(w_refs, mine)

    @pl.when(expert == 0)
    def _():
        normed = rms_norm(get(x_ref), get(gain_ref))
        gate0, gate1 = pair_gates(dot_nt(get(wr_ref), normed), get(erow_ref), ROW)
        hit0, hit1 = route_masks(get(prow_ref), rows)
        gate_rows = axis_sum(keep(hit0, gate0) + keep(hit1, gate1), COL)
        dys = select_rows(hot(hit0 | hit1), get(dx_ref)) * gate_rows
        put(dys_out, dys)
        tail = jnp.zeros((blk, width), BF16)
        dys_s[:rows] = dys.astype(BF16)
        dys_s[rows:] = tail
        xs_s[:rows] = own_first(get(xs_ref), mine)
        xs_s[rows:] = tail
        fill(dxs_s, 0)

    def body(at):
        xs = xs_s[pl.ds(at, blk)]
        dys = dys_s[pl.ds(at, blk)]

        def gradients(core):
            gate = dot_nt(weights.gate(core), xs)
            up = dot_nt(weights.up(core), xs)
            return glu_bwd(gate, up, dot_nt(weights.down(core), dys))

        parts = []

        def back(core, made):
            d_gate, d_up, _ = made
            parts.extend([dot_tn(d_gate, weights.gate(core)), dot_tn(d_up, weights.up(core))])

        staggered(weights.cores, gradients, back)
        dxs_s[pl.ds(at, blk)] = functools.reduce(jnp.add, parts)

    expert_rows(off, expert, blk, body)

    @pl.when(expert == pl.num_programs(0) - 1)
    def _():
        x = get(x_ref)
        dx = get(dx_ref)
        gain = get(gain_ref)
        normed = rms_norm(x, gain)
        logits = dot_nt(normed, get(wr_ref))
        experts = get(ecol_ref)
        gate0, gate1 = pair_gates(logits, experts, COL)
        d_gate0 = axis_sum(dx * get(y0_ref), COL)
        d_gate1 = axis_sum(dx * get(y1_ref), COL)
        mean = gate0 * d_gate0 + gate1 * d_gate1
        first, second = pair_of(experts, COL)
        ids = iota(logits.shape, COL)
        d_logits = (keep(ids == first, gate0 * (d_gate0 - mean)) + keep(ids == second, gate1 * (d_gate1 - mean))).astype(BF16)
        put(dwr_out, dot_tn(d_logits, normed))
        col_id = iota((toks, rows), COL)
        slot0, slot1 = pair_of(get(pcol_ref), COL)
        d_normed = own_first(select_rows(hot((col_id == slot0) | (col_id == slot1)), dxs_s[:rows]), mine) + dot(d_logits, get(wr_ref))
        d_x, d_gain = rms_norm_bwd(x, gain, d_normed.astype(BF16).astype(F32))
        put(dx_out, dx + d_x)
        put(dg_out, d_gain)


def glu_bwd(gate, up, d_hidden):
    sig = jax.nn.sigmoid(gate)
    act = gate * sig
    d_gate = (d_hidden * up * (sig + act * (1.0 - sig))).astype(BF16)
    d_up = (d_hidden * act).astype(BF16)
    return d_gate, d_up, (act * up).astype(BF16)


def expert_specs(layer, weights):
    return [pl.BlockSpec((1, 1, *w.shape[2:]), lambda e, *_: (layer, e, 0, 0)) for w in weights]


def moe_fwd(layer, off, fs, x, gain, w_r, pos_row, pos_col, exp_col, weights, rows):
    toks, width = x.shape
    blk = LANES
    tok_out = jax.ShapeDtypeStruct((toks, width), F32)
    out_shapes = (tok_out, jax.ShapeDtypeStruct((rows, width), BF16), tok_out, tok_out)
    small = [x, gain, w_r, pos_row, pos_col, exp_col]
    return pl.pallas_call(
        functools.partial(moe_fwd_kernel, rows=rows, blk=blk),
        out_shape=out_shapes,
        grid_spec=pltpu.PrefetchScalarGridSpec(
            num_scalar_prefetch=2,
            grid=(w_r.shape[ROW],),
            in_specs=[whole(a.shape) for a in small] + expert_specs(layer, weights),
            out_specs=tuple(whole(s.shape) for s in out_shapes),
            scratch_shapes=[pltpu.VMEM((rows + blk, width), BF16), pltpu.VMEM((rows + blk, width), F32)],
        ),
        compiler_params=params(48),
        cost_estimate=cost(30, 45),
        name="moe_fwd",
    )(off, fs, *small, *weights)


def moe_bwd(layer, off, fs, dx, x, gain, w_r, pos_row, pos_col, exp_row, exp_col, y0, y1, xs, weights, rows):
    toks, width = x.shape
    blk = LANES
    small = [dx, x, gain, w_r, pos_row, pos_col, exp_row, exp_col, y0, y1, xs]
    out_shapes = tuple(jax.ShapeDtypeStruct((count, width), F32) for count in (toks, rows, w_r.shape[ROW], 1))
    buffer = pltpu.VMEM((rows + blk, width), BF16)
    return pl.pallas_call(
        functools.partial(moe_bwd_kernel, rows=rows, blk=blk),
        out_shape=out_shapes,
        grid_spec=pltpu.PrefetchScalarGridSpec(
            num_scalar_prefetch=2,
            grid=(w_r.shape[ROW],),
            in_specs=[whole(a.shape) for a in small] + expert_specs(layer, weights),
            out_specs=tuple(whole(s.shape) for s in out_shapes),
            scratch_shapes=[buffer, buffer, pltpu.VMEM((rows + blk, width), F32)],
        ),
        compiler_params=params(60),
        cost_estimate=cost(50, 50),
        name="moe_bwd",
    )(off, fs, *small, *weights)


def expert_dw_kernel(off, fs, lr_ref, xs_hbm, dys_hbm, *refs, blk, alias):
    w_refs, masters, refs = refs[:6], refs[6:9], refs[12 if alias else 9 :]
    outs, (xbuf, dbuf, sems) = refs[:3], refs[3:]
    expert = pl.program_id(0)
    seqs = xs_hbm.shape[0]
    half = outs[0].shape[-1]
    lr = get(lr_ref)
    mine = fs[0]
    weights = ExpertWeights(w_refs, mine)

    def copies(e, slot, act):
        at = 0
        for s in range(seqs):
            start = pl.multiple_of(off[s, e], TILE)
            count = pl.multiple_of(off[s, e + 1] - off[s, e], TILE)
            target = pl.ds(pl.multiple_of(at, TILE), count)

            @pl.when(count > 0)
            def _():
                for k, (hbm, buf) in enumerate(((xs_hbm, xbuf), (dys_hbm, dbuf))):
                    act(pltpu.make_async_copy(hbm.at[s, pl.ds(start, count)], buf.at[slot, target], sems.at[slot, k]))

            at = at + count
        return at

    slot = lax.rem(expert, 2)

    @pl.when(expert == 0)
    def _():
        copies(0, 0, lambda copy: copy.start())

    @pl.when(expert + 1 < pl.num_programs(0))
    def _():
        copies(expert + 1, 1 - slot, lambda copy: copy.start())

    total = pl.multiple_of(copies(expert, slot, lambda copy: copy.wait()), TILE)
    for buf in (xbuf, dbuf):
        buf[slot, pl.ds(total, blk)] = jnp.zeros((blk, buf.shape[2]), buf.dtype)

    def block(i, bases):
        rows = pl.ds(pl.multiple_of(i * blk, blk), blk)
        xs = own_first(xbuf[slot, rows], mine)
        dys = dbuf[slot, rows].astype(BF16)
        own, xs_t, dys_t = xs[:, :half], xs.T, dys.T

        def gradients(core):
            return glu_bwd(dot(weights.gate(core), xs_t), dot(weights.up(core), xs_t), dot(weights.down(core), dys_t))

        def take(which, part, grad):
            outs[which][0, 0, part] = bases[which][0, 0, part] - lr * grad

        def add(core, made):
            d_gate, d_up, hidden = made
            part = weights.rows_of(core)
            take(0, part, dot(d_gate, own))
            take(1, part, dot(d_up, own))
            if core is weights.cores[0]:
                take(2, slice(None), dot(hidden, dys))

        staggered(weights.cores, gradients, add)

    block(0, masters)

    def more(i, carry):
        block(i, outs)
        return carry

    lax.fori_loop(1, (total + blk - 1) // blk, more, 0)


def expert_dw(layer, off, fs, lr, xs, dys, weights, masters, prev):
    seqs, _, width = xs.shape
    experts = masters[0].shape[1]
    blk = 2 * LANES
    most = seqs * width + blk
    any_spec = pl.BlockSpec(memory_space=pl.ANY)
    specs = expert_specs(layer, masters)
    alias = prev is not None
    in_specs = [whole(lr.shape), any_spec, any_spec] + expert_specs(layer, weights) + specs
    in_specs += [any_spec] * 3 if alias else []
    first_prev = len(in_specs) - 1
    return pl.pallas_call(
        functools.partial(expert_dw_kernel, blk=blk, alias=alias),
        out_shape=tuple(jax.ShapeDtypeStruct(m.shape, F32) for m in masters),
        grid_spec=pltpu.PrefetchScalarGridSpec(
            num_scalar_prefetch=2,
            grid=(experts,),
            in_specs=in_specs,
            out_specs=tuple(specs),
            scratch_shapes=[
                pltpu.VMEM((2, most, width), BF16),
                pltpu.VMEM((2, most, width), F32),
                pltpu.SemaphoreType.DMA((2, 2)),
            ],
        ),
        input_output_aliases={first_prev + k: k for k in range(3)} if alias else {},
        compiler_params=params(62),
        cost_estimate=cost(60, 150),
        name="expert_dw",
    )(off, fs, lr, xs, dys, *weights, *masters, *(prev or ()))


def head_kernel(fs, x_ref, gain_ref, lab_ref, wa_ref, wb_ref, fin_out, lse_out, dx_out, dg_out, loss_out, fin_s, top_s, sum_s, pick_s, acc_s, *, tokens_all):
    sweep = pl.program_id(0)
    step = pl.program_id(1)
    last = pl.num_programs(1) - 1
    tile = wa_ref.shape[ROW]
    mine = fs[0]
    parts = pieces(tile, HEAD_PIECE)

    @pl.when((sweep == 0) & (step == 0))
    def _():
        fin = rms_norm(get(x_ref), get(gain_ref))
        put(fin_out, fin)
        put(fin_s, own_first(fin, mine).T)
        fill(top_s, NEG)
        fill(sum_s, 0)
        fill(pick_s, 0)
        fill(acc_s, 0)

    def logits_of(part):
        return dot(both_cores((wa_ref, wb_ref), *part), get(fin_s)) * LOG2E

    def take_sums(part, logits):
        grouped = sublane_groups(logits)
        old = get(top_s)
        new = jnp.maximum(old, jnp.max(grouped, axis=ROW))
        put(sum_s, get(sum_s) * jnp.exp2(old - new) + jnp.sum(jnp.exp2(grouped - new), axis=ROW))
        put(top_s, new)

    @pl.when(sweep == 0)
    def _():
        staggered(parts, logits_of, take_sums)

    @pl.when((sweep == 0) & (step == last))
    def _():
        top = jnp.max(get(top_s), axis=ROW, keepdims=True)
        total = axis_sum(get(sum_s) * jnp.exp2(get(top_s) - top), ROW)
        put(lse_out, jnp.broadcast_to(top + jnp.log2(total), lse_out.shape))

    def gradient(part):
        logits = logits_of(part)
        prob = jnp.exp2(logits - (lse_out[:1] + jnp.log2(jnp.float32(tokens_all))))
        hit = iota(logits.shape, ROW) == get(lab_ref) - (step * tile + part[0])
        put(pick_s, get(pick_s) + jnp.sum(sublane_groups(keep(hit, logits)), axis=ROW))
        return (prob - jnp.where(hit, 1.0 / tokens_all, 0.0)).astype(BF16)

    def add_gradient(part, grad):
        put(acc_s, get(acc_s) + dot_tn(grad, both_cores((wa_ref, wb_ref), *part)))

    @pl.when(sweep == 1)
    def _():
        staggered(parts, gradient, add_gradient)

    @pl.when((sweep == 1) & (step == last))
    def _():
        per_tok = (lse_out[:1] - axis_sum(get(pick_s), ROW)) * (LN2 / tokens_all)
        put(loss_out, jnp.broadcast_to(axis_sum(per_tok, COL), loss_out.shape))
        d_fin = own_first(get(acc_s), mine).astype(BF16).astype(F32)
        d_x, d_gain = rms_norm_bwd(get(x_ref), get(gain_ref), d_fin)
        put(dx_out, d_x)
        put(dg_out, d_gain)


def head(fs, x, gain, labels, w_own, w_other, tokens_all):
    toks, width = x.shape
    vocab, half = w_own.shape
    tile = vocab // HEAD_STEPS
    out_shapes = (
        jax.ShapeDtypeStruct((toks, width), BF16),
        jax.ShapeDtypeStruct((LSE_ROWS, toks), F32),
        jax.ShapeDtypeStruct((toks, width), F32),
        jax.ShapeDtypeStruct((1, width), F32),
        jax.ShapeDtypeStruct((1, width), F32),
    )
    small = [x, gain, labels]
    w_spec = pl.BlockSpec((tile, half), lambda p, i, *_: (i, 0))
    return pl.pallas_call(
        functools.partial(head_kernel, tokens_all=tokens_all),
        out_shape=out_shapes,
        grid_spec=pltpu.PrefetchScalarGridSpec(
            num_scalar_prefetch=1,
            grid=(2, HEAD_STEPS),
            in_specs=[whole(a.shape) for a in small] + [w_spec, w_spec],
            out_specs=tuple(whole(s.shape) for s in out_shapes),
            scratch_shapes=[pltpu.VMEM((width, toks), BF16)] + [pltpu.VMEM((SUBLANES, toks), F32)] * 3 + [pltpu.VMEM((toks, width), F32)],
        ),
        compiler_params=params(56),
        cost_estimate=cost(55, 70),
        name="head_own",
    )(fs, *small, w_own, w_other)


def head_dw_kernel(fs, lr_ref, fin_ref, lse_ref, lab_ref, wa_ref, wb_ref, m_ref, new_out, oth_out, fin_s, fin_t, acc_s, *, tokens_all):
    tile, half = wa_ref.shape
    seqs = fin_s.shape[0]
    mine = fs[0]
    base = (mine * pl.num_programs(0) + pl.program_id(0)) * tile
    parts = pieces(tile, DW_PIECE)
    fill(acc_s, 0)
    fill(oth_out, 0)

    @pl.when(pl.program_id(0) == 0)
    def _():
        for s in range(seqs):
            fin = own_first(fin_ref[s], mine)
            fin_s[s] = fin
            fin_t[s] = fin.T

    def body(s, carry):
        lse = lse_ref[s, :1] + jnp.log2(jnp.float32(tokens_all))
        lab = lab_ref[s] - base

        def gradient(part):
            logits = dot(both_cores((wa_ref, wb_ref), *part), fin_t[s]) * LOG2E
            hit = iota(logits.shape, ROW) == lab - part[0]
            return (jnp.exp2(logits - lse) - jnp.where(hit, 1.0 / tokens_all, 0.0)).astype(BF16)

        def add_gradient(part, grad):
            rows = slice(*part)
            acc_s[rows] += dot(grad, fin_s[s, :, :half])
            oth_out[rows] += dot(grad, fin_s[s, :, half:])

        staggered(parts, gradient, add_gradient)
        return carry

    lax.fori_loop(0, seqs, body, 0)
    put(new_out, get(m_ref) - get(lr_ref) * get(acc_s))


def head_dw(fs, lr, fin, lse, labels, w_own, w_other, master, tokens_all):
    seqs, toks, width = fin.shape
    vocab, half = master.shape
    steps = HEAD_STEPS // 2
    tile = vocab // HEAD_STEPS
    spec = pl.BlockSpec((tile, half), lambda i, f: (f[0] * steps + i, 0))
    small = [lr, fin, lse, labels]
    return pl.pallas_call(
        functools.partial(head_dw_kernel, tokens_all=tokens_all),
        out_shape=(jax.ShapeDtypeStruct((vocab, half), F32), jax.ShapeDtypeStruct((steps * tile, half), F32)),
        grid_spec=pltpu.PrefetchScalarGridSpec(
            num_scalar_prefetch=1,
            grid=(steps,),
            in_specs=[whole(a.shape) for a in small] + [spec] * 3,
            out_specs=(spec, pl.BlockSpec((tile, half), lambda i, *_: (i, 0))),
            scratch_shapes=[
                pltpu.VMEM((seqs, toks, width), BF16),
                pltpu.VMEM((seqs, width, toks), BF16),
                pltpu.VMEM((tile, half), F32),
            ],
        ),
        compiler_params=params(60),
        cost_estimate=cost(140, 70),
        name="head_dw",
    )(fs, *small, w_own, w_other, master)


def head_upd_kernel(fs, lr_ref, grad_ref, m_ref, prev_ref, new_out):
    put(new_out, get(m_ref) - get(lr_ref) * get(grad_ref))


def head_upd(fs, lr, grad, master, prev):
    vocab, half = master.shape
    steps = HEAD_STEPS // 2
    tile = vocab // HEAD_STEPS
    spec = pl.BlockSpec((tile, half), lambda i, f: ((1 - f[0]) * steps + i, 0))
    return pl.pallas_call(
        head_upd_kernel,
        out_shape=jax.ShapeDtypeStruct((vocab, half), F32),
        grid_spec=pltpu.PrefetchScalarGridSpec(
            num_scalar_prefetch=1,
            grid=(steps,),
            in_specs=[whole(lr.shape), pl.BlockSpec((tile, half), lambda i, *_: (i, 0)), spec, pl.BlockSpec(memory_space=pl.ANY)],
            out_specs=spec,
        ),
        input_output_aliases={4: 0},
        compiler_params=params(48),
        cost_estimate=cost(15, 50),
        name="head_upd",
    )(fs, lr, grad, master, prev)


def embed_upd_kernel(bounds, keys, perm, lr_ref, rows_ref, m_ref, new_out, wide_s):
    step = pl.program_id(0)
    rows = m_ref.shape[0]

    @pl.when(step == 0)
    def _():
        put(wide_s, get(rows_ref).astype(F32) * get(lr_ref))

    put(new_out, get(m_ref))

    def body(j, carry):
        at = new_out.at[pl.ds(keys[j] - step * rows, 1)]
        put(at, get(at) - get(wide_s.at[pl.ds(perm[j], 1)]))
        return carry

    lax.fori_loop(bounds[step], bounds[step + 1], body, 0)


def embed_upd(bounds, keys, perm, lr, grads, master, rows):
    vocab, width = master.shape
    return pl.pallas_call(
        embed_upd_kernel,
        out_shape=jax.ShapeDtypeStruct((vocab, width), F32),
        grid_spec=pltpu.PrefetchScalarGridSpec(
            num_scalar_prefetch=3,
            grid=(vocab // rows,),
            in_specs=[
                whole(lr.shape),
                whole(grads.shape),
                pl.BlockSpec((rows, width), lambda i, *_: (i, 0)),
            ],
            out_specs=pl.BlockSpec((rows, width), lambda i, *_: (i, 0)),
            scratch_shapes=[pltpu.VMEM(grads.shape, F32)],
        ),
        compiler_params=params(48),
        cost_estimate=cost(25, 66),
        name="embed_upd",
    )(bounds, keys, perm, lr, grads, master)


def small_upd_kernel(lr_ref, *refs, layers):
    reduced, refs = refs[:layers], refs[layers:]
    masters, outs, loss_out = refs[: len(refs) // 2], refs[len(refs) // 2 : -1], refs[-1]
    lr = get(lr_ref)
    for l, grads in enumerate(reduced):
        half = masters[0].shape[1]
        wide = grads.shape[COL]
        at = 0
        for master, out in list(zip(masters, outs))[:4]:
            count = master.shape[2]
            out[l] = master[l] - lr * grads[:half, at : at + count]
            at += count

        def small(i):
            return grads[half + i * half // wide : half + i * half // wide + 1, i * half % wide : i * half % wide + half]

        router, gain_attn, gain_mlp, gain_final = list(zip(masters, outs))[4:]
        experts = router[0].shape[1]
        for i in range(experts):
            row = slice(i, i + 1)
            router[1][l, row] = router[0][l, row] - lr * small(i)
        own = slice(l, l + 1)
        for i, (master, out) in enumerate((gain_attn, gain_mlp)):
            out[own] = master[own] - lr * small(experts + i)
        if l == 0:
            put(gain_final[1], get(gain_final[0]) - lr * small(experts + 2))
            put(loss_out, small(experts + 3))


def small_upd(lr, reduced, masters):
    half = masters[0].shape[1]
    args = [lr, *reduced, *masters]
    out_shapes = [jax.ShapeDtypeStruct(m.shape, F32) for m in masters] + [jax.ShapeDtypeStruct((1, half), F32)]
    return pl.pallas_call(
        functools.partial(small_upd_kernel, layers=len(reduced)),
        out_shape=out_shapes,
        grid=(1,),
        in_specs=[whole(a.shape) for a in args],
        out_specs=[whole(o.shape) for o in out_shapes],
        compiler_params=params(48),
        cost_estimate=cost(4, 10),
        name="small_upd",
    )(*args)


def rope_tables(positions):
    inv_freq = ROPE_THETA ** (-jnp.arange(0, HEAD_DIM, 2, dtype=F32) / HEAD_DIM)
    angle = positions.astype(F32)[:, None] * inv_freq
    cos, sin = jnp.cos(angle), jnp.sin(angle)
    return jnp.concatenate([cos, cos], axis=COL), jnp.concatenate([-sin, sin], axis=COL)


def half_turn(x):
    return pltpu.roll(x, HEAD_DIM // 2, COL)


def rope(x, cos, sin):
    return x * cos + half_turn(x) * sin


def rope_bwd(dx, cos, sin):
    return dx * cos + half_turn(dx * sin)


def qkv_heads(x, gain, weights, cos, sin, q_width):
    normed = rms_norm(x, gain)
    all_heads = jnp.split(dot(normed, weights), weights.shape[COL] // HEAD_DIM, axis=COL)
    count = q_width // HEAD_DIM
    queries = [rope(q, cos, sin).astype(BF16) for q in all_heads[:count]]
    key, value = all_heads[count:]
    return normed, queries, rope(key, cos, sin).astype(BF16), value.astype(BF16)


def attn_probs(query, key):
    scores = dot_nt(query, key) * HEAD_DIM ** -0.5
    scores = jnp.where(iota(scores.shape, ROW) >= iota(scores.shape, COL), scores, NEG)
    raised = jnp.exp(scores - jnp.max(scores, axis=COL, keepdims=True))
    return raised / axis_sum(raised, COL)


def attn_fwd_kernel(x_ref, gain_ref, cos_ref, sin_ref, w_ref, out_ref, *, q_width, in_width):
    x = get(x_ref)
    weights = get(w_ref).reshape(x.shape[COL], -1)
    _, queries, key, value = qkv_heads(x, get(gain_ref), weights[:, :in_width], get(cos_ref), get(sin_ref), q_width)
    mixed = [dot(attn_probs(query, key).astype(BF16), value).astype(BF16) for query in queries]
    put(out_ref, x + dot(jnp.concatenate(mixed, axis=COL), weights[:, in_width:]))


def attn_bwd_kernel(dx_ref, x_ref, gain_ref, cos_ref, sin_ref, dwr_ref, dgm_ref, dgf_ref, loss_ref, w_ref, dx_out, dw_out, *, q_width, in_width):
    x = get(x_ref)
    d_out = get(dx_ref)
    gain, cos, sin = get(gain_ref), get(cos_ref), get(sin_ref)
    weights = get(w_ref).reshape(x.shape[COL], -1)
    half = x.shape[COL] // 2
    normed, queries, key, value = qkv_heads(x, gain, weights[:, :in_width], cos, sin, q_width)
    d_proj = d_out.astype(BF16)
    d_mixed = jnp.split(dot_nt(d_proj, weights[:, in_width:]).astype(BF16), len(queries), axis=COL)
    mixed, d_heads = [], []
    d_key = d_value = None
    for query, d_mix in zip(queries, d_mixed):
        probs = attn_probs(query, key)
        rounded = probs.astype(BF16)
        mixed.append(dot(rounded, value).astype(BF16))
        d_probs = dot_nt(d_mix, value)
        d_scores = (probs * (d_probs - axis_sum(d_probs * probs, COL)) * HEAD_DIM ** -0.5).astype(BF16)
        d_heads.append(rope_bwd(dot(d_scores, key), cos, sin).astype(BF16))
        more_key, more_value = dot_tn(d_scores, query), dot_tn(rounded, d_mix)
        d_key = more_key if d_key is None else d_key + more_key
        d_value = more_value if d_value is None else d_value + more_value
    d_heads += [rope_bwd(d_key, cos, sin).astype(BF16), d_value.astype(BF16)]
    d_in = jnp.concatenate(d_heads, axis=COL)
    d_weights = jnp.concatenate([dot_tn(normed, d_in), dot_tn(jnp.concatenate(mixed, axis=COL), d_proj)], axis=COL)
    d_x, d_gain = rms_norm_bwd(x, gain, dot_nt(d_in, weights[:, :in_width]).astype(BF16).astype(F32))
    put(dx_out, d_out + d_x)
    for core, d_half in enumerate(pair_of(d_weights, ROW)):
        dw_out[core, :half] = d_half
    small = jnp.concatenate([get(dwr_ref), d_gain, get(dgm_ref), get(dgf_ref), get(loss_ref)], axis=ROW)
    per_row = d_weights.shape[COL] // half
    for i in range(small.shape[ROW]):
        row, at = half + i // per_row, i % per_row * half
        for core, part in enumerate(pair_of(small[i : i + 1], COL)):
            dw_out[core, row : row + 1, at : at + half] = part


def attn_specs(arrays, w_all, layer):
    spec = pl.BlockSpec((2, 1, *w_all.shape[2:]), lambda i: (0, layer, 0, 0))
    return [whole(a.shape) for a in arrays] + [spec]


def attn_fwd(layer, x, gain, cos, sin, w_all, q_width, in_width):
    small = [x, gain, cos, sin]
    return pl.pallas_call(
        functools.partial(attn_fwd_kernel, q_width=q_width, in_width=in_width),
        out_shape=jax.ShapeDtypeStruct(x.shape, F32),
        grid=(1,),
        in_specs=attn_specs(small, w_all, layer),
        out_specs=whole(x.shape),
        compiler_params=params(48),
        cost_estimate=cost(8, 5),
        name="attn_fwd",
    )(*small, w_all)


def attn_bwd(layer, dx, x, gain, cos, sin, d_router, d_mlp, d_final, loss, w_all, q_width, in_width):
    small = [dx, x, gain, cos, sin, d_router, d_mlp, d_final, loss]
    half, wide = w_all.shape[2:]
    tail = -(-(d_router.shape[ROW] + 4) // (wide // half) // SUBLANES) * SUBLANES
    grads = jax.ShapeDtypeStruct((2, half + tail, wide), F32)
    return pl.pallas_call(
        functools.partial(attn_bwd_kernel, q_width=q_width, in_width=in_width),
        out_shape=(jax.ShapeDtypeStruct(x.shape, F32), grads),
        grid=(1,),
        in_specs=attn_specs(small, w_all, layer),
        out_specs=(whole(x.shape), whole(grads.shape)),
        compiler_params=params(60),
        cost_estimate=cost(15, 10),
        name="attn_bwd",
    )(*small, w_all)


def routing(experts_of, experts):
    toks = experts_of.shape[0]
    hot = (experts_of[:, :, None] == jnp.arange(experts, dtype=I32)).astype(F32)
    both = hot[:, 0] + hot[:, 1]
    before = iota((toks, toks), 0) > iota((toks, toks), 1)
    ahead = dot(before.astype(BF16), both.astype(BF16))
    counts = jnp.sum(both, axis=0).astype(I32)
    padded = (counts + TILE - 1) // TILE * TILE
    upto = iota((experts + 1, experts), 0) > iota((experts + 1, experts), 1)
    starts = jnp.sum(jnp.where(upto, padded[None, :], 0), axis=1)
    place = starts[:experts].astype(F32) + ahead
    return jnp.sum(hot * place[:, None, :], axis=2).astype(I32), starts


def after(x, earlier):
    return lax.optimization_barrier((x, earlier))[0]


def solution(mesh):
    device_count = mesh.shape['rep'] * mesh.shape['fsdp']
    both = ('rep', 'fsdp')
    batch_spec = P(both)
    layer_spec = P(None, 'fsdp')
    expert_spec = P(None, None, 'fsdp')
    param_specs = (P('fsdp'), layer_spec, layer_spec, layer_spec, layer_spec, layer_spec, layer_spec, layer_spec, expert_spec, expert_spec, expert_spec, P('fsdp'), P('fsdp'))
    in_specs = (batch_spec, batch_spec, batch_spec, P(None, both), P()) + param_specs
    out_specs = param_specs + (P(),)

    def step(tok_ids, tok_labels, tok_pos, expert_idx, learn_rate, embedding, w_query, w_key, w_value, w_attn_out, g_attn, g_mlp, w_router, w_gate, w_up, w_down, g_final, w_head):
        layers, half, q_width = w_query.shape
        kv_width = w_key.shape[2]
        width = 2 * half
        toks = tok_ids.shape[1]
        experts = w_router.shape[2]
        tokens_all = toks * device_count
        vocab_share = embedding.shape[0]
        rows = 2 * toks + experts * TILE
        me = lax.axis_index('fsdp')
        pair = lax.axis_index('rep')
        fs = jnp.stack([me, pair]).astype(I32)
        lr = learn_rate.reshape(1, 1)
        swap = [(0, 1), (1, 0)]

        m_gate = jnp.swapaxes(w_gate, 2, 3)
        m_up = jnp.swapaxes(w_up, 2, 3)
        m_head = w_head.T
        router_t = jnp.swapaxes(w_router, 1, 2)

        experts_of = expert_idx[:, 0]
        placed = [routing(experts_of[l], experts) for l in range(layers)]
        starts = jnp.stack([s for _, s in placed])
        ints = jnp.concatenate([tok_ids[0], tok_labels[0], starts.reshape(-1)]).astype(F32)
        misc = jnp.concatenate([router_t.reshape(layers * experts, half), g_attn, g_mlp, g_final[None]])
        misc = misc.astype(BF16).astype(F32).reshape(-1)
        packed = jnp.concatenate([misc, ints])
        n_misc = misc.shape[0]
        packed = jnp.pad(packed, (0, KNOWN - packed.shape[0])).reshape(-1, LANES)
        known = lax.all_gather(packed, both).reshape(device_count, -1)
        two = lax.dynamic_slice_in_dim(known, pair * 2, 2, 0)[:, :n_misc].reshape(2, -1, half)
        misc_all = jnp.concatenate([two[0], two[1]], axis=1)
        w_r = [misc_all[l * experts : (l + 1) * experts].astype(BF16) for l in range(layers)]
        base = layers * experts
        gain_attn = [misc_all[base + l][None] for l in range(layers)]
        gain_mlp = [misc_all[base + layers + l][None] for l in range(layers)]
        gain_final = misc_all[base + 2 * layers][None]
        known_ints = known[:, n_misc : n_misc + ints.shape[0]].astype(I32)
        ids_all = known_ints[:, :toks]
        labels_all = known_ints[:, toks : 2 * toks]
        starts_all = known_ints[:, 2 * toks :].reshape(device_count, layers, experts + 1)

        attn_pack = jnp.concatenate([w_query, w_key, w_value, w_attn_out], axis=2).astype(BF16)
        attn_all = lax.all_gather(attn_pack, 'fsdp')

        def with_partner(x):
            rounded = x.astype(BF16)
            return rounded, lax.ppermute(rounded, 'fsdp', swap)

        expert_w = with_partner(after(m_gate, packed)) + with_partner(after(m_up, packed)) + with_partner(after(w_down, packed))

        partner_ids = lax.dynamic_index_in_dim(ids_all, pair * 2 + 1 - me, 0, keepdims=False)
        wanted = jnp.concatenate([tok_ids[0], partner_ids]) - me * vocab_share
        taken = jnp.take(embedding, jnp.clip(wanted, 0, vocab_share - 1), axis=0).astype(BF16)
        sent = lax.ppermute(taken[toks:], 'fsdp', swap)
        head_w = with_partner(after(m_head, taken))
        is_mine = (wanted[:toks] >= 0) & (wanted[:toks] < vocab_share)
        x = jnp.where(is_mine[:, None], taken[:toks], sent).astype(F32)

        tables = rope_tables(tok_pos[0])
        widths = (q_width, q_width + 2 * kv_width)

        xs_all, kept = [], []
        for l in range(layers):
            mid = attn_fwd(l, x, gain_attn[l], *tables, attn_all, *widths)
            pos, start = placed[l]
            out, xs, y0, y1 = moe_fwd(l, start, fs, mid, gain_mlp[l], w_r[l], pos.T, pos, experts_of[l], expert_w, rows)
            kept.append((x, mid, xs, y0, y1))
            xs_all.append(lax.all_gather(xs, both))
            x = out

        fin, lse, dx, d_final, loss = head(fs, x, gain_final, tok_labels, *head_w, tokens_all)
        fin_all = lax.all_gather(fin, both)
        lse_all = lax.all_gather(lse, both)

        dys_all = [None] * layers
        reduced = [None] * layers
        for l in reversed(range(layers)):
            x, mid, xs, y0, y1 = kept[l]
            pos, start = placed[l]
            dx, dys, d_router, d_mlp = moe_bwd(l, start, fs, dx, mid, gain_mlp[l], w_r[l], pos.T, pos, experts_of[l].T, experts_of[l], y0, y1, xs, expert_w, rows)
            dys_all[l] = lax.all_gather(dys, both)
            dx, grads = attn_bwd(l, dx, x, gain_attn[l], *tables, d_router, d_mlp, d_final, loss, attn_all, *widths)
            reduced[l] = lax.psum(lax.psum_scatter(grads, 'fsdp', scatter_dimension=0, tiled=False), 'rep')

        d_rows = lax.all_gather(dx.astype(BF16), both).reshape(tokens_all, width)

        fin_all = after(fin_all, dx)
        new_head, other_grad = head_dw(fs, lr, fin_all, lse_all, labels_all[:, None], *head_w, m_head, tokens_all)
        other_grad = lax.ppermute(other_grad, 'fsdp', swap)
        dys_all[1] = after(dys_all[1], new_head)
        new_experts = None
        for l in reversed(range(layers)):
            new_experts = expert_dw(l, starts_all[:, l], fs, lr, xs_all[l], dys_all[l], expert_w, (m_gate, m_up, w_down), new_experts)

        small_masters = (w_query, w_key, w_value, w_attn_out, router_t, g_attn, g_mlp, g_final[None])
        *small_new, total_loss = small_upd(lr, reduced, small_masters)
        new_head = head_upd(fs, lr, after(other_grad, new_experts[0]), m_head, new_head)

        block = 1336
        local_id = ids_all.reshape(-1) - me * vocab_share
        key = jnp.where((local_id >= 0) & (local_id < vocab_share), local_id, vocab_share)
        keys, perm = lax.sort((key, lax.iota(I32, tokens_all)), num_keys=1)
        edges = jnp.arange(vocab_share // block + 1, dtype=I32) * block
        bounds = jnp.sum(key[None, :] < edges[:, None], axis=1).astype(I32)
        new_embedding = embed_upd(bounds, keys, perm, lr, after(d_rows, new_experts[0]), embedding, block)

        new_query, new_key, new_value, new_attn_out, new_router, new_g_attn, new_g_mlp, new_final = small_new
        new_gate, new_up, new_down = new_experts
        return (new_embedding, new_query, new_key, new_value, new_attn_out, new_g_attn, new_g_mlp, jnp.swapaxes(new_router, 1, 2),
                jnp.swapaxes(new_gate, 2, 3), jnp.swapaxes(new_up, 2, 3), new_down, new_final[0], new_head.T, total_loss[0, 0])

    return jax.shard_map(step, mesh=mesh, in_specs=in_specs, out_specs=out_specs, check_vma=False)
```
